128 devices in a mesh: dp: 16 (over z, x), cent: 8 (over y, core).
Axes of the slice: x: 4, y: 4, z: 4, core: 2. Of those that a mesh axis runs over, the one named last changes fastest.
Arguments:
- points: float32 [32768, 512], P('dp'), may hold values from -30 to 30
- centroids: float32 [32768, 512], P('cent'), may hold values from -5 to 5
Outputs:
- new_centroids: float32 [32768, 512], P('cent')
The draws below stay inside these ranges and needn't reach their ends.
All inputs are finite; a program needn't handle non-finite values.
Results may differ from the reference program's by a relative error of at most 0.0061.
Values sent between devices are 32-bit elements; how exact they have to be, the bound alone decides.
A program may use at most 128 MiB of HBM per device.

```python
import jax
import jax.numpy as jnp
from jax import lax

D = 512
K = 32768
POINTS = 32768


def shared_centroids(key):
    base = jnp.clip(jax.random.normal(jax.random.fold_in(key, 11), (K, D), jnp.float32), -5.0, 5.0)
    return base


def draw_centroids(key, part):
    return shared_centroids(key)


def draw_points(key, part):
    base = jnp.clip(jax.random.normal(jax.random.fold_in(key, 12), (POINTS, D), jnp.float32), -6.0, 6.0)
    cents = shared_centroids(key)
    picks = 2 * jax.random.randint(jax.random.fold_in(key, 15), (POINTS,), 0, K // 2)
    level = jax.random.randint(jax.random.fold_in(key, 16), (POINTS,), 0, 4).astype(jnp.float32)
    target = 110.0 + 60.0 * level
    factor = 0.5 * (target / jnp.sqrt(jnp.float32(D)) + 1.0)
    aligned = factor[:, None] * cents[picks]
    chosen = jnp.arange(POINTS) % 64 == 0
    base = jnp.where(chosen[:, None], aligned, base)
    return jnp.clip(base, -30.0, 30.0)


def setup_inputs(seed: int = 0) -> dict:
    splits = jax.random.split(jax.random.key(seed), 3)
    points = draw_points(jax.random.fold_in(splits[2], 71), 0)
    centroids = draw_centroids(jax.random.fold_in(splits[2], 71), 0)
    return {"points": points, "centroids": centroids}


def reference(points, centroids):
    cent_half = centroids.astype(jnp.bfloat16)
    sq_norm = lax.optimization_barrier(jnp.sum(centroids * centroids, axis=1))
    scale = 1.0 / jnp.sqrt(jnp.float32(D))
    block_rows = min(1024, POINTS)
    blocks = points.reshape(POINTS // block_rows, block_rows, D)

    def step(carry, block):
        weighted, counts = carry
        point_half = block.astype(jnp.bfloat16)
        inner = jnp.dot(point_half, cent_half.T, preferred_element_type=jnp.float32)
        logit = (2.0 * inner - sq_norm[None, :]) * scale
        top = lax.optimization_barrier(jnp.max(logit, axis=1, keepdims=True))
        expo = jnp.exp(logit - top)
        total = lax.optimization_barrier(jnp.sum(expo, axis=1, keepdims=True))
        resp = (expo / total).astype(jnp.bfloat16)
        weighted = weighted + jnp.dot(resp.T, point_half, preferred_element_type=jnp.float32)
        counts = counts + lax.optimization_barrier(jnp.sum(resp.astype(jnp.float32), axis=0))
        return ((weighted, counts), None)
    start = (jnp.zeros((K, D), jnp.float32), jnp.zeros((K,), jnp.float32))
    (weighted, counts), unused = lax.scan(step, start, blocks)
    return (weighted + centroids) / (counts + 1.0)[:, None]
```

```python
import functools

import jax
import jax.numpy as jnp
from jax import lax
from jax.experimental import pallas as pl
from jax.experimental.pallas import tpu as pltpu
from jax.sharding import PartitionSpec as P

MESH = pl.DeviceIdType.MESH
F32, BF16 = jnp.float32, jnp.bfloat16
LOG2E = 1.4426950408889634


def kernel(
    n_cent,
    points,
    cents,
    out,
    ph,
    pstage,
    cstage,
    ch,
    sqb,
    logit0,
    logit1,
    expo,
    mtop,
    msum,
    factor,
    stat,
    statr,
    row,
    w,
    got,
    r1,
    r2,
    t1,
    t2,
    cfin,
    cnt,
    cntx,
    cntz,
    ssem,
    rsem,
    lsem,
):
    n_points, width = ph.shape
    chunk = ch.shape[0]
    n_chunk = mtop.shape[0]
    tile = logit0.shape[1]
    n_tile = n_points // tile
    rows = w.shape[4]
    scale = LOG2E / width**0.5

    dp = lax.axis_index("dp")
    ce = lax.axis_index("cent")
    x, z = lax.rem(dp, 4), lax.div(dp, 4)

    def at_x(d):
        return (z * 4 + lax.rem(x + d, 4), ce)

    def at_z(d):
        return (lax.rem(z + d, 4) * 4 + x, ce)

    def at_cent(d):
        return (dp, lax.rem(ce + d, n_cent))

    peers = [at_x(d) for d in (1, 2, 3)] + [at_z(d) for d in (1, 2, 3)]
    peers += [at_cent(d) for d in range(1, n_cent)]
    barrier = pltpu.get_barrier_semaphore()
    for peer in peers:
        pl.semaphore_signal(barrier, inc=1, device_id=peer, device_id_type=MESH)

    used = [0]
    sent = []

    def send(src, dst, dev):
        i = used[0]
        used[0] += 1
        copy = pltpu.make_async_remote_copy(
            src_ref=src,
            dst_ref=dst,
            send_sem=ssem.at[i],
            recv_sem=rsem.at[i],
            device_id=dev,
            device_id_type=MESH,
        )
        copy.start()
        sent.append(copy)
        return copy

    part = n_points // 4

    def load_points(i):
        return pltpu.make_async_copy(
            points.at[pl.ds(i * part, part)], pstage.at[i % 2], lsem.at[i % 2]
        )

    def load_cents(i, slot):
        return pltpu.make_async_copy(
            cents.at[pl.ds(i * chunk, chunk)], cstage.at[slot], lsem.at[2 + slot]
        )

    load_points(0).start()
    load_points(1).start()
    load_cents(0, 0).start()
    load_cents(1, 1).start()
    for i in range(4):
        load_points(i).wait()
        ph[pl.ds(i * part, part), :] = pstage[i % 2].astype(BF16)
        if i + 2 < 4:
            load_points(i + 2).start()

    def first(t, logit):
        at = pl.multiple_of(t * tile, tile)
        inner = lax.dot_general(
            ch[...], ph[pl.ds(at, tile), :], (((1,), (1,)), ((), ())),
            preferred_element_type=F32,
        )
        value = inner * (2.0 * scale) - jnp.concatenate([sqb[...]] * (tile // 128), axis=1)
        logit[...] = value
        return jnp.max(value, axis=0, keepdims=True)

    def second(c, t, logit, high):
        at = pl.multiple_of(t * tile, tile)
        e = jnp.exp2(logit[...] - high)
        base = pl.multiple_of(c * chunk, chunk)
        expo[pl.ds(base, chunk), pl.ds(at, tile)] = e.astype(BF16)
        mtop[c, :, pl.ds(at, tile)] = high
        msum[c, :, pl.ds(at, tile)] = jnp.sum(e, axis=0, keepdims=True)

    def on_chunk(c, carry):
        slot = lax.rem(c, 2)
        load_cents(c, slot).wait()
        value = cstage[slot]
        ch[...] = value.astype(BF16)
        sqb[...] = jnp.broadcast_to(
            jnp.sum(value * value, axis=1, keepdims=True) * scale, sqb.shape
        )

        @pl.when(c + 2 < n_chunk)
        def _():
            load_cents(c + 2, slot).start()

        high = first(0, logit0)

        def pair(j, high):
            other = first(2 * j + 1, logit1)
            second(c, 2 * j, logit0, high)
            high = first(lax.rem(2 * j + 2, n_tile), logit0)
            second(c, 2 * j + 1, logit1, other)
            return high

        lax.fori_loop(0, n_tile // 2, pair, high)
        return carry

    lax.fori_loop(0, n_chunk, on_chunk, 0)

    top = functools.reduce(jnp.maximum, [mtop[c] for c in range(n_chunk)])
    total = sum(msum[c] * jnp.exp2(mtop[c] - top) for c in range(n_chunk))
    for i in range(n_points // 128):
        stat[0, i : i + 1, :] = top[:, i * 128 : (i + 1) * 128]
        stat[1, i : i + 1, :] = total[:, i * 128 : (i + 1) * 128]
    pl.semaphore_wait(barrier, len(peers))
    copies = [send(stat, statr.at[d - 1], at_cent(d)) for d in range(1, n_cent)]

    us, vs = (x, z), (z, x)
    fins = []
    for c in range(2):
        for h in range(2):
            at = ((c * 4 + us[c]) * 2 + h) * (4 * rows) + vs[c] * rows
            fins.append(
                pltpu.make_async_copy(
                    cents.at[pl.ds(pl.multiple_of(at, rows), rows)],
                    cfin.at[c, h],
                    lsem.at[4 + 2 * c + h],
                )
            )
            fins[-1].start()

    for copy in copies:
        copy.wait_recv()
    tops = [stat[0]] + [statr[d, 0] for d in range(n_cent - 1)]
    sums = [stat[1]] + [statr[d, 1] for d in range(n_cent - 1)]
    high = functools.reduce(jnp.maximum, tops)
    inverse = 1.0 / sum(s * jnp.exp2(t - high) for t, s in zip(tops, sums))
    for i in range(n_points // 128):
        row[0, :, i * 128 : (i + 1) * 128] = high[i : i + 1, :]
        row[1, :, i * 128 : (i + 1) * 128] = inverse[i : i + 1, :]
    for c in range(n_chunk):
        factor[c] = jnp.exp2(mtop[c] - row[0]) * row[1]

    def produce(c, bu, h):
        block = (c * 4 + bu) * 2 + h
        at = pl.multiple_of(block * (4 * rows), 4 * rows)
        group = lax.div(block * (4 * rows), chunk)
        acc = jnp.zeros((4 * rows, width), F32)
        count = jnp.zeros((4 * rows, 128), F32)
        step = n_points // 4
        for k in range(4):
            cols = slice(k * step, (k + 1) * step)
            resp = (expo[pl.ds(at, 4 * rows), cols].astype(F32) * factor[group, :, cols]).astype(BF16)
            acc += jnp.dot(resp, ph[cols, :], preferred_element_type=F32)
            wide = resp.astype(F32)
            for l in range(step // 128):
                count += wide[:, l * 128 : (l + 1) * 128]
        w[c, bu, h] = acc.reshape(4, rows, width)
        line = jnp.sum(count.T, axis=0, keepdims=True)
        for b in range(4):
            cnt[block, b, :, :rows] = line[:, b * rows : (b + 1) * rows]

    ups = (at_x(1), at_z(1))
    downs = (at_x(3), at_z(3))
    u = [[lax.rem(us[c] + d, 4) for d in range(4)] for c in range(2)]
    v = [[lax.rem(vs[c] + d, 4) for d in range(4)] for c in range(2)]
    order = (2, 1, 3, 0)

    a_up, a_dn, b_up, b_dn = {}, {}, {}, {}
    for c in range(2):
        produce(c, u[c][2], 0)
        for d in order:
            b = v[c][d]
            a_up[c, d] = send(w.at[c, u[c][2], 0, b], r1.at[c, 0, b], ups[c])
        produce(c, u[c][2], 1)
        for d in order:
            b = v[c][d]
            a_dn[c, d] = send(w.at[c, u[c][2], 1, b], r1.at[c, 1, b], downs[c])
    own = []
    for c in range(2):
        produce(c, u[c][1], 1)
        own.append(send(w.at[c, u[c][1], 1], r2.at[c, 0, 1], ups[c]))
        produce(c, u[c][3], 0)
        own.append(send(w.at[c, u[c][3], 0], r2.at[c, 1, 0], downs[c]))
    for c in range(2):
        produce(c, u[c][1], 0)
        produce(c, u[c][3], 1)
    for c in range(2):
        produce(c, u[c][0], 0)
        produce(c, u[c][0], 1)
    copies = [send(cnt, cntx.at[d - 1], at_x(d)) for d in (1, 2, 3)]

    for d in order:
        for c in range(2):
            b = v[c][d]
            a_up[c, d].wait_recv()
            w[c, u[c][1], 0, b] += r1[c, 0, b]
            b_up[c, d] = send(w.at[c, u[c][1], 0, b], r2.at[c, 0, 0, b], ups[c])
            a_dn[c, d].wait_recv()
            w[c, u[c][3], 1, b] += r1[c, 1, b]
            b_dn[c, d] = send(w.at[c, u[c][3], 1, b], r2.at[c, 1, 1, b], downs[c])
    for copy in copies:
        copy.wait_recv()
    for copy in copies:
        copy.wait_send()
    sent[:] = [copy for copy in sent if all(copy is not done for done in copies)]
    cnt[...] = cnt[...] + cntx[0] + cntx[1] + cntx[2]
    copies = [send(cnt, cntz.at[d - 1], at_z(d)) for d in (1, 2, 3)]
    for copy in own:
        copy.wait_recv()

    ups2, downs2 = ups[::-1], downs[::-1]
    s_up, s_dn, q = {}, {}, []
    for d in order:
        for c in range(2):
            b, me = v[c][d], us[c]
            b_up[c, d].wait_recv()
            b_dn[c, d].wait_recv()
            for h in range(2):
                w[c, me, h, b] += r2[c, 0, h, b] + r2[c, 1, h, b]
            if d == 2:
                s_up[c] = send(w.at[c, me, 0, b], t1.at[c, 0], ups2[c])
                s_dn[c] = send(w.at[c, me, 1, b], t1.at[c, 1], downs2[c])
            if d == 1:
                q.append(send(w.at[c, me, 1, b], t2.at[c, 0, 1], ups2[c]))
            if d == 3:
                q.append(send(w.at[c, me, 0, b], t2.at[c, 1, 0], downs2[c]))
    for c in range(2):
        me = us[c]
        s_up[c].wait_recv()
        w[c, me, 0, v[c][1]] += t1[c, 0]
        q.append(send(w.at[c, me, 0, v[c][1]], t2.at[c, 0, 0], ups2[c]))
        s_dn[c].wait_recv()
        w[c, me, 1, v[c][3]] += t1[c, 1]
        q.append(send(w.at[c, me, 1, v[c][3]], t2.at[c, 1, 1], downs2[c]))
    for copy in copies + q:
        copy.wait_recv()
    for copy in fins:
        copy.wait()

    g_up, g_dn = {}, {}
    for c in range(2):
        me, b = us[c], vs[c]
        for h in range(2):
            block = (c * 4 + me) * 2 + h
            line = cnt[block, b] + cntz[0, block, b] + cntz[1, block, b] + cntz[2, block, b]
            count = jnp.broadcast_to(line, (128, 128)).T[:rows]
            count = jnp.concatenate([count] * (width // 128), axis=1)
            value = w[c, me, h, b] + t2[c, 0, h] + t2[c, 1, h]
            got[c, me, h, b] = (value + cfin[c, h]) / (count + 1.0)
        mine = got.at[c, me, :, b]
        g_up[c] = send(mine, mine, ups2[c])
        g_dn[c] = send(mine, mine, downs2[c])

    h_up, h_dn, f_up, f_dn = {}, {}, {}, {}

    def spread(c, d):
        piece = got.at[c, us[c], :, v[c][d]]
        h_up[c, d] = send(piece, piece, ups[c])
        h_dn[c, d] = send(piece, piece, downs[c])

    def save(piece_of):
        pltpu.make_async_copy(piece_of(got), piece_of(out), lsem.at[8]).start()

    for c in range(2):
        spread(c, 0)
        save(lambda ref: ref.at[c, us[c], :, vs[c]])
    for c in range(2):
        me = us[c]
        g_up[c].wait_recv()
        piece = got.at[c, me, 0, v[c][3]]
        f_up[c] = send(piece, piece, ups2[c])
        spread(c, 3)
        save(lambda ref: ref.at[c, me, :, v[c][3]])
        g_dn[c].wait_recv()
        piece = got.at[c, me, 1, v[c][1]]
        f_dn[c] = send(piece, piece, downs2[c])
        spread(c, 1)
        save(lambda ref: ref.at[c, me, :, v[c][1]])
    k_up, k_dn = {}, {}

    def onward(c, d):
        b = v[c][d]
        h_up[c, d].wait_recv()
        piece = got.at[c, u[c][3], 0, b]
        k_up[c, d] = send(piece, piece, ups[c])
        save(lambda ref: ref.at[c, u[c][3], :, b])
        h_dn[c, d].wait_recv()
        piece = got.at[c, u[c][1], 1, b]
        k_dn[c, d] = send(piece, piece, downs[c])
        save(lambda ref: ref.at[c, u[c][1], :, b])

    for c in range(2):
        onward(c, 0)
    for c in range(2):
        f_up[c].wait_recv()
        f_dn[c].wait_recv()
        spread(c, 2)
        save(lambda ref: ref.at[c, us[c], :, v[c][2]])
    for d in (3, 1, 2):
        for c in range(2):
            onward(c, d)
    for d in (0, 3, 1, 2):
        for c in range(2):
            k_up[c, d].wait_recv()
            k_dn[c, d].wait_recv()
            save(lambda ref: ref.at[c, u[c][2], :, v[c][d]])
    for copy in sent:
        copy.wait_send()
    pltpu.make_async_copy(got, out, lsem.at[8]).wait()


def body(points, centroids):
    n_points, width = points.shape
    n_rows = centroids.shape[0]
    n_cent = lax.axis_size("cent")
    chunk, tile = n_rows // 4, 512
    rows = n_rows // 64
    pieces = (2, 4, 2, 4, rows, width)
    n_copies = 2 * 44 + (n_cent - 1) + 6
    vm = pltpu.VMEM
    flat = (n_rows // chunk, 1, n_points)
    scratch = [
        vm((n_points, width), BF16),
        vm((2, n_points // 4, width), F32),
        vm((2, chunk, width), F32),
        vm((chunk, width), BF16),
        vm((chunk, 128), F32),
        vm((chunk, tile), F32),
        vm((chunk, tile), F32),
        vm((n_rows, n_points), BF16),
        vm(flat, F32),
        vm(flat, F32),
        vm(flat, F32),
        vm((2, n_points // 128, 128), F32),
        vm((n_cent - 1, 2, n_points // 128, 128), F32),
        vm((2, 1, n_points), F32),
        vm(pieces, F32),
        vm(pieces, F32),
        vm((2, 2, 4, rows, width), F32),
        vm((2, 2, 2, 4, rows, width), F32),
        vm((2, 2, rows, width), F32),
        vm((2, 2, 2, rows, width), F32),
        vm((2, 2, rows, width), F32),
        vm((16, 4, 1, 128), F32),
        vm((3, 16, 4, 1, 128), F32),
        vm((3, 16, 4, 1, 128), F32),
        pltpu.SemaphoreType.DMA((n_copies,)),
        pltpu.SemaphoreType.DMA((n_copies,)),
        pltpu.SemaphoreType.DMA((9,)),
    ]
    result = pl.pallas_call(
        functools.partial(kernel, n_cent),
        out_shape=jax.ShapeDtypeStruct(pieces, F32),
        in_specs=[pl.BlockSpec(memory_space=pl.ANY)] * 2,
        out_specs=pl.BlockSpec(memory_space=pl.ANY),
        scratch_shapes=scratch,
        compiler_params=pltpu.CompilerParams(
            collective_id=0, has_side_effects=True, vmem_limit_bytes=67_000_000
        ),
    )(points, centroids)
    return result.reshape(n_rows, width)


def solution(mesh):
    placed = (P("dp", None), P("cent", None))
    return jax.shard_map(
        body, mesh=mesh, in_specs=placed, out_specs=P("cent", None), check_vma=False
    )
```

```python
import functools

import jax
import jax.numpy as jnp
from jax import lax
from jax.experimental import pallas as pl
from jax.experimental.pallas import tpu as pltpu
from jax.sharding import PartitionSpec as P

MESH = pl.DeviceIdType.MESH
F32, BF16 = jnp.float32, jnp.bfloat16
LOG2E = 1.4426950408889634


def kernel(
    n_cent,
    points,
    cents,
    got,
    ph,
    cstage,
    ch,
    sqb,
    logit0,
    logit1,
    expo,
    mtop,
    msum,
    factor,
    stat,
    statr,
    row,
    w,
    r1,
    r2,
    t1,
    t2,
    cfin,
    cnt,
    cntx,
    cntz,
    ssem,
    rsem,
    lsem,
):
    n_points, width = ph.shape
    chunk = ch.shape[1]
    n_chunk = mtop.shape[0]
    tile = logit0.shape[1]
    n_tile = n_points // tile
    rows = w.shape[4]
    scale = LOG2E / width**0.5

    dp = lax.axis_index("dp")
    ce = lax.axis_index("cent")
    x, z = lax.rem(dp, 4), lax.div(dp, 4)

    def at_x(d):
        return (z * 4 + lax.rem(x + d, 4), ce)

    def at_z(d):
        return (lax.rem(z + d, 4) * 4 + x, ce)

    def at_cent(d):
        return (dp, lax.rem(ce + d, n_cent))

    peers = [at_x(d) for d in (1, 2, 3)] + [at_z(d) for d in (1, 2, 3)]
    peers += [at_cent(d) for d in range(1, n_cent)]
    barrier = pltpu.get_barrier_semaphore()
    for peer in peers:
        pl.semaphore_signal(barrier, inc=1, device_id=peer, device_id_type=MESH)

    used = [0]
    sent = []

    def slots(n):
        used[0] += n
        return used[0] - n

    def remote(i, src, dst, dev):
        return pltpu.make_async_remote_copy(
            src_ref=src,
            dst_ref=dst,
            send_sem=ssem.at[i],
            recv_sem=rsem.at[i],
            device_id=dev,
            device_id_type=MESH,
        )

    def send(src, dst, dev):
        copy = remote(slots(1), src, dst, dev)
        copy.start()
        sent.append(copy)
        return copy

    part = n_points // 4

    def load_points(i):
        return pltpu.make_async_copy(
            points.at[i], w.at[0, i], lsem.at[i]
        )

    def load_cents(i):
        slot = lax.rem(i, 2)
        return pltpu.make_async_copy(
            cents.at[pl.ds(i * chunk, chunk)], cstage.at[slot], lsem.at[4 + slot]
        )

    load_points(0).start()
    load_cents(0).start()
    for i in range(1, 4):
        load_points(i).start()
    load_cents(1).start()

    def round_cents(i):
        slot = lax.rem(i, 2)
        value = cstage[slot]
        ch[slot] = value.astype(BF16)
        sqb[slot] = jnp.broadcast_to(
            jnp.sum(value * value, axis=1, keepdims=True) * scale, (chunk, 128)
        )

    def first(c, t, logit):
        slot = lax.rem(c, 2)
        inner = lax.dot_general(
            ch[slot], ph[t * tile : (t + 1) * tile, :], (((1,), (1,)), ((), ())),
            preferred_element_type=F32,
        )
        value = inner * (2.0 * scale) - jnp.concatenate([sqb[slot]] * (tile // 128), axis=1)
        logit[...] = value
        return jnp.max(value, axis=0, keepdims=True)

    def second(c, t, logit, high):
        at = slice(t * tile, (t + 1) * tile)
        e = jnp.exp2(logit[...] - high)
        base = pl.multiple_of(c * chunk, chunk)
        expo[pl.ds(base, chunk), at] = e.astype(BF16)
        mtop[c, :, at] = high
        msum[c, :, at] = jnp.sum(e, axis=0, keepdims=True)

    logits = (logit0, logit1)

    def on_chunk(c, high, last):
        if not last:
            load_cents(c + 1).wait()

            @pl.when(c + 2 < n_chunk)
            def _():
                load_cents(c + 2).start()

        for t in range(n_tile):
            if t + 1 < n_tile:
                after = first(c, t + 1, logits[(t + 1) % 2])
                if t == 0 and not last:
                    round_cents(c + 1)
            elif not last:
                after = first(c + 1, 0, logits[(t + 1) % 2])
            second(c, t, logits[t % 2], high)
            high = after
        return high

    for i in range(4):
        load_points(i).wait()
        ph[i * part : (i + 1) * part, :] = w[0, i].reshape(part, width).astype(BF16)
        if i == 0:
            load_cents(0).wait()
            round_cents(0)
    high = first(0, 0, logit0)
    high = lax.fori_loop(0, n_chunk - 1, lambda c, high: on_chunk(c, high, False), high)
    on_chunk(n_chunk - 1, high, True)

    top = functools.reduce(jnp.maximum, [mtop[c] for c in range(n_chunk)])
    total = sum(msum[c] * jnp.exp2(mtop[c] - top) for c in range(n_chunk))
    for i in range(n_points // 128):
        stat[0, i : i + 1, :] = top[:, i * 128 : (i + 1) * 128]
        stat[1, i : i + 1, :] = total[:, i * 128 : (i + 1) * 128]
    pl.semaphore_wait(barrier, len(peers))
    copies = [send(stat, statr.at[d - 1], at_cent(d)) for d in range(1, n_cent)]

    us, vs = (x, z), (z, x)
    fins = []
    for c in range(2):
        for h in range(2):
            at = ((c * 4 + us[c]) * 2 + h) * (4 * rows) + vs[c] * rows
            fins.append(
                pltpu.make_async_copy(
                    cents.at[pl.ds(pl.multiple_of(at, rows), rows)],
                    cfin.at[c, h],
                    lsem.at[6 + 2 * c + h],
                )
            )
            fins[-1].start()

    for copy in copies:
        copy.wait_recv()
    tops = [stat[0]] + [statr[d, 0] for d in range(n_cent - 1)]
    sums = [stat[1]] + [statr[d, 1] for d in range(n_cent - 1)]
    high = functools.reduce(jnp.maximum, tops)
    inverse = 1.0 / sum(s * jnp.exp2(t - high) for t, s in zip(tops, sums))
    for i in range(n_points // 128):
        row[0, :, i * 128 : (i + 1) * 128] = high[i : i + 1, :]
        row[1, :, i * 128 : (i + 1) * 128] = inverse[i : i + 1, :]
    for c in range(n_chunk):
        factor[c] = jnp.exp2(mtop[c] - row[0]) * row[1]

    def produce(c, bu, h):
        block = (c * 4 + bu) * 2 + h
        at = pl.multiple_of(block * (4 * rows), 4 * rows)
        group = lax.div(block * (4 * rows), chunk)
        acc = jnp.zeros((4 * rows, width), F32)
        count = jnp.zeros((4 * rows, 128), F32)
        step = n_points // 4
        for k in range(4):
            cols = slice(k * step, (k + 1) * step)
            resp = (expo[pl.ds(at, 4 * rows), cols].astype(F32) * factor[group, :, cols]).astype(BF16)
            acc += jnp.dot(resp, ph[cols, :], preferred_element_type=F32)
            wide = resp.astype(F32)
            for l in range(step // 128):
                count += wide[:, l * 128 : (l + 1) * 128]
        w[c, bu, h] = acc.reshape(4, rows, width)
        line = jnp.sum(count.T, axis=0, keepdims=True)
        for b in range(4):
            cnt[block, b, :, :rows] = line[:, b * rows : (b + 1) * rows]

    ups = (at_x(1), at_z(1))
    downs = (at_x(3), at_z(3))
    u = [[lax.rem(us[c] + d, 4) for d in range(4)] for c in range(2)]
    v = [[lax.rem(vs[c] + d, 4) for d in range(4)] for c in range(2)]
    order = (2, 1, 3, 0)

    def place(c):
        return x * (1 - c) + z * c, z * (1 - c) + x * c

    def along(c, d):
        return (lax.rem(z + c * d, 4) * 4 + lax.rem(x + (1 - c) * d, 4), ce)

    far, near = slots(16), slots(4)

    def far_copy(c, h, k):
        here, other = place(c)
        b = lax.rem(other + order[k], 4)
        return remote(
            far + (c * 2 + h) * 4 + k,
            w.at[c, lax.rem(here + 2, 4), h, b],
            r1.at[c, h, b],
            along(c, 1 + 2 * h),
        )

    def near_copy(c, h):
        here, _ = place(c)
        d = 3 - 2 * h
        return remote(
            near + c * 2 + h, w.at[c, lax.rem(here + d, 4), h], r2.at[c, 1 - h, h], along(c, d)
        )

    def farthest(i, carry):
        c, h = lax.rem(i, 2), lax.div(i, 2)
        produce(c, lax.rem(place(c)[0] + 2, 4), h)
        for k in range(4):
            far_copy(c, h, k).start()
        return carry

    def nearest(i, carry):
        c, h = lax.rem(i, 2), 1 - lax.div(i, 2)
        produce(c, lax.rem(place(c)[0] + 3 - 2 * h, 4), h)
        near_copy(c, h).start()
        return carry

    def others(i, carry):
        c, h, mine = lax.rem(i, 2), lax.rem(lax.div(i, 2), 2), lax.div(i, 4)
        produce(c, lax.rem(place(c)[0] + (1 - mine) * (1 + 2 * h), 4), h)
        return carry

    lax.fori_loop(0, 4, farthest, 0)
    lax.fori_loop(0, 4, nearest, 0)
    lax.fori_loop(0, 8, others, 0)
    a_up, a_dn, b_up, b_dn = {}, {}, {}, {}
    for c in range(2):
        for k in range(4):
            a_up[c, order[k]], a_dn[c, order[k]] = far_copy(c, 0, k), far_copy(c, 1, k)
    own = [near_copy(c, h) for c in range(2) for h in range(2)]
    sent.extend(own + list(a_up.values()) + list(a_dn.values()))
    copies = [send(cnt, cntx.at[d - 1], at_x(d)) for d in (1, 2, 3)]

    for d in order:
        for c in range(2):
            b = v[c][d]
            a_up[c, d].wait_recv()
            w[c, u[c][1], 0, b] += r1[c, 0, b]
            b_up[c, d] = send(w.at[c, u[c][1], 0, b], r2.at[c, 0, 0, b], ups[c])
            a_dn[c, d].wait_recv()
            w[c, u[c][3], 1, b] += r1[c, 1, b]
            b_dn[c, d] = send(w.at[c, u[c][3], 1, b], r2.at[c, 1, 1, b], downs[c])
    for copy in copies:
        copy.wait_recv()
    for copy in copies:
        copy.wait_send()
    sent[:] = [copy for copy in sent if all(copy is not done for done in copies)]
    cnt[...] = cnt[...] + cntx[0] + cntx[1] + cntx[2]
    copies = [send(cnt, cntz.at[d - 1], at_z(d)) for d in (1, 2, 3)]
    for copy in own:
        copy.wait_recv()

    ups2, downs2 = ups[::-1], downs[::-1]
    s_up, s_dn, q = {}, {}, []
    for d in order:
        for c in range(2):
            b, me = v[c][d], us[c]
            b_up[c, d].wait_recv()
            b_dn[c, d].wait_recv()
            for h in range(2):
                w[c, me, h, b] += r2[c, 0, h, b] + r2[c, 1, h, b]
            if d == 2:
                s_up[c] = send(w.at[c, me, 0, b], t1.at[c, 0], ups2[c])
                s_dn[c] = send(w.at[c, me, 1, b], t1.at[c, 1], downs2[c])
            if d == 1:
                q.append(send(w.at[c, me, 1, b], t2.at[c, 0, 1], ups2[c]))
            if d == 3:
                q.append(send(w.at[c, me, 0, b], t2.at[c, 1, 0], downs2[c]))
    for c in range(2):
        me = us[c]
        s_up[c].wait_recv()
        w[c, me, 0, v[c][1]] += t1[c, 0]
        q.append(send(w.at[c, me, 0, v[c][1]], t2.at[c, 0, 0], ups2[c]))
        s_dn[c].wait_recv()
        w[c, me, 1, v[c][3]] += t1[c, 1]
        q.append(send(w.at[c, me, 1, v[c][3]], t2.at[c, 1, 1], downs2[c]))
    for copy in copies + q:
        copy.wait_recv()
    for copy in fins:
        copy.wait()

    g_up, g_dn = {}, {}
    for c in range(2):
        me, b = us[c], vs[c]
        for h in range(2):
            block = (c * 4 + me) * 2 + h
            line = cnt[block, b] + cntz[0, block, b] + cntz[1, block, b] + cntz[2, block, b]
            count = jnp.broadcast_to(line, (128, 128)).T[:rows]
            count = jnp.concatenate([count] * (width // 128), axis=1)
            value = w[c, me, h, b] + t2[c, 0, h] + t2[c, 1, h]
            got[c, me, h, b] = (value + cfin[c, h]) / (count + 1.0)
        mine = got.at[c, me, :, b]
        g_up[c] = send(mine, mine, ups2[c])
        g_dn[c] = send(mine, mine, downs2[c])

    h_up, h_dn, f_up, f_dn = {}, {}, {}, {}

    def spread(c, d):
        piece = got.at[c, us[c], :, v[c][d]]
        h_up[c, d] = send(piece, piece, ups[c])
        h_dn[c, d] = send(piece, piece, downs[c])

    for c in range(2):
        spread(c, 0)
    for c in range(2):
        me = us[c]
        g_up[c].wait_recv()
        piece = got.at[c, me, 0, v[c][3]]
        f_up[c] = send(piece, piece, ups2[c])
        spread(c, 3)
        g_dn[c].wait_recv()
        piece = got.at[c, me, 1, v[c][1]]
        f_dn[c] = send(piece, piece, downs2[c])
        spread(c, 1)
    k_up, k_dn = {}, {}

    def onward(c, d):
        b = v[c][d]
        h_up[c, d].wait_recv()
        piece = got.at[c, u[c][3], 0, b]
        k_up[c, d] = send(piece, piece, ups[c])
        h_dn[c, d].wait_recv()
        piece = got.at[c, u[c][1], 1, b]
        k_dn[c, d] = send(piece, piece, downs[c])

    for c in range(2):
        onward(c, 0)
    for c in range(2):
        f_up[c].wait_recv()
        f_dn[c].wait_recv()
        spread(c, 2)
    for d in (3, 1, 2):
        for c in range(2):
            onward(c, d)
    for d in (0, 3, 1, 2):
        for c in range(2):
            k_up[c, d].wait_recv()
            k_dn[c, d].wait_recv()
    for copy in sent:
        copy.wait_send()


def store(got, out, sem):
    copies = [
        pltpu.make_async_copy(got.at[c, pl.ds(2 * h, 2)], out.at[c, pl.ds(2 * h, 2)], sem.at[2 * c + h])
        for c in range(2)
        for h in range(2)
    ]
    for copy in copies:
        copy.start()
    for copy in copies:
        copy.wait()


def body(points, centroids):
    n_points, width = points.shape
    n_rows = centroids.shape[0]
    n_cent = lax.axis_size("cent")
    chunk, tile = n_rows // 4, 512
    rows = n_rows // 64
    pieces = (2, 4, 2, 4, rows, width)
    n_copies = 2 * 46 + (n_cent - 1) + 6
    vm = pltpu.VMEM
    flat = (n_rows // chunk, 1, n_points)
    scratch = [
        vm((n_points, width), BF16),
        vm((2, chunk, width), F32),
        vm((2, chunk, width), BF16),
        vm((2, chunk, 128), F32),
        vm((chunk, tile), F32),
        vm((chunk, tile), F32),
        vm((n_rows, n_points), BF16),
        vm(flat, F32),
        vm(flat, F32),
        vm(flat, F32),
        vm((2, n_points // 128, 128), F32),
        vm((n_cent - 1, 2, n_points // 128, 128), F32),
        vm((2, 1, n_points), F32),
        vm(pieces, F32),
        vm((2, 2, 4, rows, width), F32),
        vm((2, 2, 2, 4, rows, width), F32),
        vm((2, 2, rows, width), F32),
        vm((2, 2, 2, rows, width), F32),
        vm((2, 2, rows, width), F32),
        vm((16, 4, 1, 128), F32),
        vm((3, 16, 4, 1, 128), F32),
        vm((3, 16, 4, 1, 128), F32),
        pltpu.SemaphoreType.DMA((n_copies,)),
        pltpu.SemaphoreType.DMA((n_copies,)),
        pltpu.SemaphoreType.DMA((10,)),
    ]
    result = pl.pallas_call(
        functools.partial(kernel, n_cent),
        out_shape=pltpu.VMEM(pieces, F32),
        in_specs=[pl.BlockSpec(memory_space=pl.ANY)] * 2,
        out_specs=pl.BlockSpec(memory_space=pltpu.VMEM),
        scratch_shapes=scratch,
        compiler_params=pltpu.CompilerParams(
            collective_id=0, has_side_effects=True, vmem_limit_bytes=50 * 2**20
        ),
    )(points.reshape(4, 2, 4, n_points // 32, width), centroids)
    saved = pl.pallas_call(
        store,
        out_shape=jax.ShapeDtypeStruct(pieces, F32),
        in_specs=[pl.BlockSpec(memory_space=pltpu.VMEM)],
        out_specs=pl.BlockSpec(memory_space=pl.ANY),
        scratch_shapes=[pltpu.SemaphoreType.DMA((4,))],
        compiler_params=pltpu.CompilerParams(vmem_limit_bytes=2**20),
    )(result)
    return saved.reshape(n_rows, width)


def solution(mesh):
    placed = (P("dp", None), P("cent", None))
    return jax.shard_map(
        body, mesh=mesh, in_specs=placed, out_specs=P("cent", None), check_vma=False
    )
```

```python
import functools

import jax
import jax.numpy as jnp
from jax import lax
from jax.experimental import pallas as pl
from jax.experimental.pallas import tpu as pltpu
from jax.sharding import PartitionSpec as P

MESH = pl.DeviceIdType.MESH
F32, BF16 = jnp.float32, jnp.bfloat16
LOG2E = 1.4426950408889634


def kernel(
    n_cent,
    points,
    cents,
    got,
    ph,
    cstage,
    ch,
    sqb,
    logit0,
    logit1,
    expo,
    mtop,
    msum,
    factor,
    stat,
    statr,
    row,
    w,
    r1,
    r2,
    t1,
    t2,
    cfin,
    cnt,
    cntx0,
    cntx1,
    cntz,
    ssem,
    rsem,
    lsem,
):
    n_points, width = ph.shape
    chunk = ch.shape[1]
    n_chunk = mtop.shape[0]
    tile = logit0.shape[1]
    n_tile = n_points // tile
    rows = w.shape[4]
    scale = LOG2E / width**0.5

    dp = lax.axis_index("dp")
    ce = lax.axis_index("cent")
    x, z = lax.rem(dp, 4), lax.div(dp, 4)

    def at_x(d):
        return (z * 4 + lax.rem(x + d, 4), ce)

    def at_z(d):
        return (lax.rem(z + d, 4) * 4 + x, ce)

    def at_cent(d):
        return (dp, lax.rem(ce + d, n_cent))

    peers = [at_x(d) for d in (1, 2, 3)] + [at_z(d) for d in (1, 2, 3)]
    peers += [at_cent(d) for d in range(1, n_cent)]
    barrier = pltpu.get_barrier_semaphore()
    for peer in peers:
        pl.semaphore_signal(barrier, inc=1, device_id=peer, device_id_type=MESH)

    used = [0]
    sent = []

    def slots(n):
        used[0] += n
        return used[0] - n

    def remote(i, src, dst, dev):
        return pltpu.make_async_remote_copy(
            src_ref=src,
            dst_ref=dst,
            send_sem=ssem.at[i],
            recv_sem=rsem.at[i],
            device_id=dev,
            device_id_type=MESH,
        )

    def send(src, dst, dev):
        copy = remote(slots(1), src, dst, dev)
        copy.start()
        sent.append(copy)
        return copy

    part = n_points // 4

    def load_points(i):
        return pltpu.make_async_copy(
            points.at[i], w.at[0, i], lsem.at[i]
        )

    def load_cents(i):
        slot = lax.rem(i, 2)
        return pltpu.make_async_copy(
            cents.at[pl.ds(i * chunk, chunk)], cstage.at[slot], lsem.at[4 + slot]
        )

    load_points(0).start()
    load_cents(0).start()
    load_cents(1).start()
    for i in range(1, 4):
        load_points(i).start()

    def round_points(i):
        load_points(i).wait()
        ph[i * part : (i + 1) * part, :] = w[0, i].reshape(part, width).astype(BF16)

    def round_cents(i):
        load_cents(i).wait()
        value = cstage[i % 2]
        ch[i] = value.astype(BF16)
        sqb[i] = jnp.broadcast_to(
            jnp.sum(value * value, axis=1, keepdims=True) * scale, (chunk, 128)
        )
        if i + 2 < n_chunk:
            load_cents(i + 2).start()

    def span(t):
        return pl.ds(pl.multiple_of(t * tile, tile), tile)

    def first(t, c, logit):
        inner = lax.dot_general(
            ch[c], ph[span(t), :], (((1,), (1,)), ((), ())), preferred_element_type=F32
        )
        value = inner * (2.0 * scale) - jnp.concatenate([sqb[c]] * (tile // 128), axis=1)
        logit[...] = value
        return jnp.max(value, axis=0, keepdims=True)

    def second(t, c, logit, high):
        e = jnp.exp2(logit[...] - high)
        expo[c * chunk : (c + 1) * chunk, span(t)] = e.astype(BF16)
        mtop[c, :, span(t)] = high
        msum[c, :, span(t)] = jnp.sum(e, axis=0, keepdims=True)

    stats = slots(n_tile * (n_cent - 1))

    def stat_copy(t, d):
        i = stats + t * (n_cent - 1) + d - 1
        return remote(i, stat.at[t], statr.at[d - 1, t], at_cent(d))

    def local_stats(t):
        tops = [mtop[c, :, span(t)] for c in range(n_chunk)]
        top = functools.reduce(jnp.maximum, tops)
        total = sum(msum[c, :, span(t)] * jnp.exp2(tops[c] - top) for c in range(n_chunk))
        for i in range(tile // 128):
            stat[t, 0, i : i + 1, :] = top[:, i * 128 : (i + 1) * 128]
            stat[t, 1, i : i + 1, :] = total[:, i * 128 : (i + 1) * 128]
        for d in range(1, n_cent):
            stat_copy(t, d).start()

    logits = (logit0, logit1)

    def on_tile(t, high, start=False, last=False):
        for c in range(n_chunk):
            after = None
            if c + 1 < n_chunk:
                after = first(t, c + 1, logits[(c + 1) % 2])
            elif not last:
                after = first(t + 1, 0, logits[(c + 1) % 2])
            if start and c + 2 < n_chunk:
                round_cents(c + 2)
            if start and c + 1 < n_tile:
                round_points(c + 1)
            second(t, c, logits[c % 2], high)
            high = after
        if start:
            pl.semaphore_wait(barrier, len(peers))
        local_stats(t)
        return high

    round_points(0)
    round_cents(0)
    high = first(0, 0, logit0)
    round_cents(1)
    high = on_tile(0, high, start=True)
    high = lax.fori_loop(1, n_tile - 1, on_tile, high)
    on_tile(n_tile - 1, high, last=True)
    sent.extend(stat_copy(t, d) for t in range(n_tile) for d in range(1, n_cent))

    def absorb(t):
        for d in range(1, n_cent):
            stat_copy(t, d).wait_recv()
        tops = [stat[t, 0]] + [statr[d, t, 0] for d in range(n_cent - 1)]
        sums = [stat[t, 1]] + [statr[d, t, 1] for d in range(n_cent - 1)]
        high = functools.reduce(jnp.maximum, tops)
        inverse = 1.0 / sum(s * jnp.exp2(t - high) for t, s in zip(tops, sums))
        for i in range(tile // 128):
            at = slice(t * tile + i * 128, t * tile + (i + 1) * 128)
            row[0, :, at] = high[i : i + 1, :]
            row[1, :, at] = inverse[i : i + 1, :]
        at = slice(t * tile, (t + 1) * tile)
        for c in range(n_chunk):
            factor[c, :, at] = jnp.exp2(mtop[c, :, at] - row[0, :, at]) * row[1, :, at]

    us, vs = (x, z), (z, x)
    fins = []
    for c in range(2):
        for h in range(2):
            at = ((c * 4 + us[c]) * 2 + h) * (4 * rows) + vs[c] * rows
            fins.append(
                pltpu.make_async_copy(
                    cents.at[pl.ds(pl.multiple_of(at, rows), rows)],
                    cfin.at[c, h],
                    lsem.at[6 + 2 * c + h],
                )
            )
            fins[-1].start()

    def produce(c, bu, h, tiles, fresh):
        block = (c * 4 + bu) * 2 + h
        at = pl.multiple_of(block * (4 * rows), 4 * rows)
        group = lax.div(block * (4 * rows), chunk)
        acc = jnp.zeros((4 * rows, width), F32)
        count = jnp.zeros((4 * rows, 128), F32)
        for t in tiles:
            cols = slice(t * tile, (t + 1) * tile)
            resp = (expo[pl.ds(at, 4 * rows), cols].astype(F32) * factor[group, :, cols]).astype(BF16)
            acc += jnp.dot(resp, ph[cols, :], preferred_element_type=F32)
            wide = resp.astype(F32)
            for l in range(tile // 128):
                count += wide[:, l * 128 : (l + 1) * 128]
        acc = acc.reshape(4, rows, width)
        w[c, bu, h] = acc if fresh else w[c, bu, h] + acc
        line = jnp.sum(count.T, axis=0, keepdims=True)
        for b in range(4):
            part = line[:, b * rows : (b + 1) * rows]
            cnt[block, b, :, :rows] = part if fresh else cnt[block, b, :, :rows] + part

    ups = (at_x(1), at_z(1))
    downs = (at_x(3), at_z(3))
    u = [[lax.rem(us[c] + d, 4) for d in range(4)] for c in range(2)]
    v = [[lax.rem(vs[c] + d, 4) for d in range(4)] for c in range(2)]
    order = (2, 1, 3, 0)

    def place(c):
        return x * (1 - c) + z * c, z * (1 - c) + x * c

    def along(c, d):
        return (lax.rem(z + c * d, 4) * 4 + lax.rem(x + (1 - c) * d, 4), ce)

    far, near = slots(16), slots(4)

    def far_copy(c, h, k):
        here, other = place(c)
        b = lax.rem(other + order[k], 4)
        return remote(
            far + (c * 2 + h) * 4 + k,
            w.at[c, lax.rem(here + 2, 4), h, b],
            r1.at[c, h, b],
            along(c, 1 + 2 * h),
        )

    def near_copy(c, h):
        here, _ = place(c)
        d = 3 - 2 * h
        return remote(
            near + c * 2 + h, w.at[c, lax.rem(here + d, 4), h], r2.at[c, 1 - h, h], along(c, d)
        )

    def begin(i, carry):
        c, h = lax.rem(i, 2), lax.div(i, 2)
        produce(c, lax.rem(place(c)[0] + 2, 4), h, range(n_tile - 1), True)
        return carry

    def farthest(i, carry):
        c, h = lax.rem(i, 2), lax.div(i, 2)
        produce(c, lax.rem(place(c)[0] + 2, 4), h, [n_tile - 1], False)
        for k in range(4):
            far_copy(c, h, k).start()
        return carry

    def nearest(i, carry):
        c, h = lax.rem(i, 2), 1 - lax.div(i, 2)
        produce(c, lax.rem(place(c)[0] + 3 - 2 * h, 4), h, range(n_tile), True)
        near_copy(c, h).start()
        return carry

    def others(i, carry):
        c, h, mine = lax.rem(i, 2), lax.rem(lax.div(i, 2), 2), lax.div(i, 4)
        produce(c, lax.rem(place(c)[0] + (1 - mine) * (1 + 2 * h), 4), h, range(n_tile), True)
        return carry

    for t in range(n_tile - 1):
        absorb(t)
    lax.fori_loop(0, 4, begin, 0)
    absorb(n_tile - 1)
    lax.fori_loop(0, 4, farthest, 0)
    lax.fori_loop(0, 4, nearest, 0)
    lax.fori_loop(0, 8, others, 0)
    a_up, a_dn, b_up, b_dn = {}, {}, {}, {}
    for c in range(2):
        for k in range(4):
            a_up[c, order[k]], a_dn[c, order[k]] = far_copy(c, 0, k), far_copy(c, 1, k)
    own = [near_copy(c, h) for c in range(2) for h in range(2)]
    sent.extend(own + list(a_up.values()) + list(a_dn.values()))
    copies = []
    for d in (1, 2, 3):
        to = lax.rem(x + d, 4)
        copies.append(send(cnt.at[pl.ds(2 * to, 2)], cntx0.at[d - 1], at_x(d)))
        copies.append(send(cnt.at[pl.ds(8, 8), to], cntx1.at[d - 1], at_x(d)))

    for d in order:
        for c in range(2):
            b = v[c][d]
            a_up[c, d].wait_recv()
            w[c, u[c][1], 0, b] += r1[c, 0, b]
            b_up[c, d] = send(w.at[c, u[c][1], 0, b], r2.at[c, 0, 0, b], ups[c])
            a_dn[c, d].wait_recv()
            w[c, u[c][3], 1, b] += r1[c, 1, b]
            b_dn[c, d] = send(w.at[c, u[c][3], 1, b], r2.at[c, 1, 1, b], downs[c])
    for copy in copies:
        copy.wait_recv()
    mine = pl.ds(2 * x, 2)
    cnt[mine] = cnt[mine] + cntx0[0] + cntx0[1] + cntx0[2]
    cnt[8:16, x] = cnt[8:16, x] + cntx1[0] + cntx1[1] + cntx1[2]
    copies = []
    for d in (1, 2, 3):
        to = lax.rem(z + d, 4)
        copies.append(send(cnt.at[mine, to], cntz.at[0, d - 1], at_z(d)))
        copies.append(send(cnt.at[pl.ds(8 + 2 * to, 2), x], cntz.at[1, d - 1], at_z(d)))
    for copy in own:
        copy.wait_recv()

    ups2, downs2 = ups[::-1], downs[::-1]
    halves = [pl.ds(q * (rows // 2), rows // 2) for q in range(2)]
    s_up, s_dn, ends = {}, {}, ([], [])

    def pass_on(c, h, d, q):
        side = h if d is None else 1 - h
        to = (ups2, downs2)[side][c]
        b = v[c][d or (1 + 2 * h)]
        ends[q].append(
            send(w.at[c, us[c], h, b, halves[q]], t2.at[c, side, h, halves[q]], to)
        )

    for d in order:
        for c in range(2):
            b, me = v[c][d], us[c]
            b_up[c, d].wait_recv()
            b_dn[c, d].wait_recv()
            for h in range(2):
                w[c, me, h, b] += r2[c, 0, h, b] + r2[c, 1, h, b]
            if d == 2:
                for q in range(2):
                    part = halves[q]
                    s_up[c, q] = send(w.at[c, me, 0, b, part], t1.at[c, 0, part], ups2[c])
                    s_dn[c, q] = send(w.at[c, me, 1, b, part], t1.at[c, 1, part], downs2[c])
            if d == 1:
                pass_on(c, 1, 1, 0)
            if d == 3:
                pass_on(c, 0, 3, 0)
    for q in range(2):
        if q == 1:
            for c in range(2):
                pass_on(c, 1, 1, 1)
                pass_on(c, 0, 3, 1)
        for c in range(2):
            me, part = us[c], halves[q]
            s_up[c, q].wait_recv()
            w[c, me, 0, v[c][1], part] += t1[c, 0, part]
            pass_on(c, 0, None, q)
            s_dn[c, q].wait_recv()
            w[c, me, 1, v[c][3], part] += t1[c, 1, part]
            pass_on(c, 1, None, q)

    for copy in copies:
        copy.wait_recv()
    for copy in fins:
        copy.wait()
    counts = {}
    for c in range(2):
        for h in range(2):
            line = cnt[(c * 4 + us[c]) * 2 + h, vs[c]]
            line = line + cntz[c, 0, h] + cntz[c, 1, h] + cntz[c, 2, h]
            counts[c, h] = jnp.broadcast_to(line, (128, 128)).T + 1.0
    g_up, g_dn, h_up, h_dn, f_up, f_dn = {}, {}, {}, {}, {}, {}
    for q in range(2):
        for copy in ends[q]:
            copy.wait_recv()
        part = halves[q]
        for c in range(2):
            me, b = us[c], vs[c]
            for h in range(2):
                count = counts[c, h][q * (rows // 2) : (q + 1) * (rows // 2)]
                count = jnp.concatenate([count] * (width // 128), axis=1)
                value = w[c, me, h, b, part] + t2[c, 0, h, part] + t2[c, 1, h, part]
                got[c, me, h, b, part] = (value + cfin[c, h, part]) / count
            mine = got.at[c, me, :, b, part]
            g_up[c, q] = send(mine, mine, ups2[c])
            g_dn[c, q] = send(mine, mine, downs2[c])
        for c in range(2):
            mine = got.at[c, us[c], :, vs[c], part]
            h_up[c, q] = send(mine, mine, ups[c])
            h_dn[c, q] = send(mine, mine, downs[c])

    e_up, e_dn = {}, {}

    def spread(c, d):
        piece = got.at[c, us[c], :, v[c][d]]
        e_up[c, d] = send(piece, piece, ups[c])
        e_dn[c, d] = send(piece, piece, downs[c])

    for c in range(2):
        me = us[c]
        g_up[c, 0].wait_recv()
        g_up[c, 1].wait_recv()
        piece = got.at[c, me, 0, v[c][3]]
        f_up[c] = send(piece, piece, ups2[c])
        spread(c, 3)
        g_dn[c, 0].wait_recv()
        g_dn[c, 1].wait_recv()
        piece = got.at[c, me, 1, v[c][1]]
        f_dn[c] = send(piece, piece, downs2[c])
        spread(c, 1)
    k_up, k_dn = {}, {}

    def onward(c, d):
        b = v[c][d]
        for copy in [h_up[c, 0], h_up[c, 1]] if d == 0 else [e_up[c, d]]:
            copy.wait_recv()
        piece = got.at[c, u[c][3], 0, b]
        k_up[c, d] = send(piece, piece, ups[c])
        for copy in [h_dn[c, 0], h_dn[c, 1]] if d == 0 else [e_dn[c, d]]:
            copy.wait_recv()
        piece = got.at[c, u[c][1], 1, b]
        k_dn[c, d] = send(piece, piece, downs[c])

    for c in range(2):
        onward(c, 0)
    for c in range(2):
        f_up[c].wait_recv()
        f_dn[c].wait_recv()
        spread(c, 2)
    for d in (3, 1, 2):
        for c in range(2):
            onward(c, d)
    for d in (0, 3, 1, 2):
        for c in range(2):
            k_up[c, d].wait_recv()
            k_dn[c, d].wait_recv()
    for copy in sent:
        copy.wait_send()


def store(got, out, sem):
    copies = [
        pltpu.make_async_copy(got.at[c, pl.ds(2 * h, 2)], out.at[c, pl.ds(2 * h, 2)], sem.at[2 * c + h])
        for c in range(2)
        for h in range(2)
    ]
    for copy in copies:
        copy.start()
    for copy in copies:
        copy.wait()


def body(points, centroids):
    n_points, width = points.shape
    n_rows = centroids.shape[0]
    n_cent = lax.axis_size("cent")
    chunk, tile = n_rows // 4, 512
    rows = n_rows // 64
    pieces = (2, 4, 2, 4, rows, width)
    n_copies = 2 * 54 + 4 * (n_cent - 1) + 12
    vm = pltpu.VMEM
    flat = (n_rows // chunk, 1, n_points)
    scratch = [
        vm((n_points, width), BF16),
        vm((2, chunk, width), F32),
        vm((n_rows // chunk, chunk, width), BF16),
        vm((n_rows // chunk, chunk, 128), F32),
        vm((chunk, tile), F32),
        vm((chunk, tile), F32),
        vm((n_rows, n_points), BF16),
        vm(flat, F32),
        vm(flat, F32),
        vm(flat, F32),
        vm((n_points // tile, 2, tile // 128, 128), F32),
        vm((n_cent - 1, n_points // tile, 2, tile // 128, 128), F32),
        vm((2, 1, n_points), F32),
        vm(pieces, F32),
        vm((2, 2, 4, rows, width), F32),
        vm((2, 2, 2, 4, rows, width), F32),
        vm((2, 2, rows, width), F32),
        vm((2, 2, 2, rows, width), F32),
        vm((2, 2, rows, width), F32),
        vm((16, 4, 1, 128), F32),
        vm((3, 2, 4, 1, 128), F32),
        vm((3, 8, 1, 128), F32),
        vm((2, 3, 2, 1, 128), F32),
        pltpu.SemaphoreType.DMA((n_copies,)),
        pltpu.SemaphoreType.DMA((n_copies,)),
        pltpu.SemaphoreType.DMA((10,)),
    ]
    result = pl.pallas_call(
        functools.partial(kernel, n_cent),
        out_shape=pltpu.VMEM(pieces, F32),
        in_specs=[pl.BlockSpec(memory_space=pl.ANY)] * 2,
        out_specs=pl.BlockSpec(memory_space=pltpu.VMEM),
        scratch_shapes=scratch,
        compiler_params=pltpu.CompilerParams(
            collective_id=0, has_side_effects=True, vmem_limit_bytes=54 * 2**20
        ),
    )(points.reshape(4, 2, 4, n_points // 32, width), centroids)
    saved = pl.pallas_call(
        store,
        out_shape=jax.ShapeDtypeStruct(pieces, F32),
        in_specs=[pl.BlockSpec(memory_space=pltpu.VMEM)],
        out_specs=pl.BlockSpec(memory_space=pl.ANY),
        scratch_shapes=[pltpu.SemaphoreType.DMA((4,))],
        compiler_params=pltpu.CompilerParams(vmem_limit_bytes=2**20),
    )(result)
    return saved.reshape(n_rows, width)


def solution(mesh):
    placed = (P("dp", None), P("cent", None))
    return jax.shard_map(
        body, mesh=mesh, in_specs=placed, out_specs=P("cent", None), check_vma=False
    )
```

```python
import functools

import jax
import jax.numpy as jnp
from jax import lax
from jax.experimental import pallas as pl
from jax.experimental.pallas import tpu as pltpu
from jax.sharding import PartitionSpec as P

MESH = pl.DeviceIdType.MESH
F32, BF16 = jnp.float32, jnp.bfloat16
LOG2E = 1.4426950408889634


def kernel(
    n_cent,
    points,
    cents,
    got,
    ph,
    pho,
    pin,
    cstage,
    ch,
    sqb,
    logit0,
    logit1,
    expo,
    mtop,
    msum,
    factor,
    stat,
    statr,
    row,
    rowo,
    w,
    x1,
    x2,
    r1,
    r2,
    t1,
    t2,
    cfin,
    cnt,
    cx0,
    cx1,
    cntz,
    ssem,
    rsem,
    lsem,
):
    n_points, width = ph.shape
    chunk = cstage.shape[1]
    n_chunk = mtop.shape[0]
    tile = logit0.shape[1]
    n_tile = n_points // tile
    rows = w.shape[2]
    scale = LOG2E / width**0.5

    dp = lax.axis_index("dp")
    ce = lax.axis_index("cent")
    x, z = lax.rem(dp, 4), lax.div(dp, 4)

    y, core = lax.div(ce, 2), lax.rem(ce, 2)

    def slot_of(x):
        return 2 * lax.rem(lax.div(x + 1, 2), 2) + lax.div(x, 2)

    half, g = lax.rem(lax.div(x + 1, 2), 2), lax.div(x, 2)
    slot = slot_of(x)
    friend = (z * 4 + x + 1 - 2 * lax.rem(x, 2), ce)
    mate = (z * 4 + 3 - x, ce)

    def at_y(d):
        return (dp, lax.rem(y + d, 4) * 2 + core)

    sibling = (dp, y * 2 + 1 - core)

    def at_x(d):
        return (z * 4 + lax.rem(x + d, 4), ce)

    def at_z(d):
        return (lax.rem(z + d, 4) * 4 + x, ce)

    def at_cent(d):
        return (dp, lax.rem(ce + d, n_cent))

    peers = [at_x(d) for d in (1, 3)] + [at_z(d) for d in (1, 2, 3)]
    peers += [at_cent(d) for d in range(1, n_cent)]
    barrier = pltpu.get_barrier_semaphore()
    for peer in peers:
        pl.semaphore_signal(barrier, inc=1, device_id=peer, device_id_type=MESH)

    used = [0]
    sent = []

    def slots(n):
        used[0] += n
        return used[0] - n

    def remote(i, src, dst, dev):
        return pltpu.make_async_remote_copy(
            src_ref=src,
            dst_ref=dst,
            send_sem=ssem.at[i],
            recv_sem=rsem.at[i],
            device_id=dev,
            device_id_type=MESH,
        )

    def send(src, dst, dev):
        copy = remote(slots(1), src, dst, dev)
        copy.start()
        sent.append(copy)
        return copy

    part = n_points // 4

    def load_points(i):
        return pltpu.make_async_copy(
            points.at[pl.ds(2 * i, 2)], w.at[pl.ds(2 * i, 2)], lsem.at[i]
        )

    def load_cents(i):
        return pltpu.make_async_copy(
            cents.at[pl.ds(i * chunk, chunk)], cstage.at[i % 2], lsem.at[4 + i % 2]
        )

    for i in range(4):
        load_points(i).start()
    load_cents(0).start()
    load_cents(1).start()

    def round_cents(i):
        value = cstage[i % 2]
        ch[i * chunk : (i + 1) * chunk, :] = value.astype(BF16)
        sqb[i * chunk : (i + 1) * chunk, :] = jnp.broadcast_to(
            jnp.sum(value * value, axis=1, keepdims=True) * scale, (chunk, 128)
        )

    def first(c, t, logit):
        at = slice(c * chunk, (c + 1) * chunk)
        inner = lax.dot_general(
            ch[at, :], ph[t * tile : (t + 1) * tile, :], (((1,), (1,)), ((), ())),
            preferred_element_type=F32,
        )
        value = inner * (2.0 * scale) - jnp.concatenate([sqb[at, :]] * (tile // 128), axis=1)
        logit[...] = value
        return jnp.max(value, axis=0, keepdims=True)

    def second(c, t, logit, high):
        at = slice(t * tile, (t + 1) * tile)
        e = jnp.exp2(logit[...] - high)
        expo[c * chunk : (c + 1) * chunk, at] = e.astype(BF16)
        mtop[c, :, at] = high
        msum[c, :, at] = jnp.sum(e, axis=0, keepdims=True)

    across = lax.rem(y + 2, 4) * 2 + core
    behind, ahead = lax.rem(y + 3, 4) * 2 + core, lax.rem(y + 1, 4) * 2 + core
    bring, go_up, go_dn, turn, side = slots(6), slots(4), slots(4), slots(2), slots(16)

    def bring_copy(i):
        if i < 4:
            return remote(bring + i, w.at[ce, i], pin.at[ce, i], friend)
        return remote(bring + i, points.at[across, i - 2], pin.at[across, i - 2], friend)

    def up_copy(i):
        return remote(go_up + i, pin.at[ce, i], pin.at[ce, i], at_y(1))

    def dn_copy(i):
        return remote(go_dn + i, pin.at[ce, i], pin.at[ce, i], at_y(3))

    def turn_copy(i):
        at, to = ((behind, at_y(1)), (ahead, at_y(3)))[i]
        return remote(turn + i, pin.at[at, i], pin.at[at, i], to)

    def side_copy(k, i):
        at = (ce, ahead, across, behind)[k]
        return remote(side + 4 * k + i, pin.at[at, i], pin.at[at, i], sibling)

    def start(copy):
        copy.start()
        sent.append(copy)

    def import_all():
        pl.semaphore_wait(barrier, len(peers))
        for i in range(6):
            bring_copy(i).start()
        sent.extend(bring_copy(i) for i in (4, 5))

    def relay(i):
        bring_copy(i).wait_recv()
        start(up_copy(i))
        start(dn_copy(i))
        start(side_copy(0, i))

    def relay_next(i):
        up_copy(i).wait_recv()
        if i == 0:
            start(turn_copy(0))
        start(side_copy(3, i))
        dn_copy(i).wait_recv()
        if i == 1:
            start(turn_copy(1))
        start(side_copy(1, i))

    def relay_far(i):
        (turn_copy(i) if i < 2 else bring_copy(i + 2)).wait_recv()
        start(side_copy(2, i))

    events = {1: import_all, 9: lambda: relay(0), 13: lambda: relay(1)}
    logits = (logit0, logit1)
    for i in range(4):
        load_points(i).wait()
        ph[i * part : (i + 1) * part, :] = w[2 * i : 2 * i + 2].reshape(part, width).astype(BF16)
        if i == 0:
            load_cents(0).wait()
            round_cents(0)
    high = first(0, 0, logit0)
    for c in range(n_chunk):
        last = c + 1 == n_chunk
        if not last:
            load_cents(c + 1).wait()
            if c + 2 < n_chunk:
                load_cents(c + 2).start()
        for t in range(n_tile):
            after = None
            if t + 1 < n_tile:
                after = first(c, t + 1, logits[(t + 1) % 2])
                if t == 0 and not last:
                    round_cents(c + 1)
            elif not last:
                after = first(c + 1, 0, logits[(t + 1) % 2])
            second(c, t, logits[t % 2], high)
            high = after
            events.get(c * n_tile + t, lambda: None)()

    stats = slots(n_cent - 1)

    def stat_copy(d):
        return remote(stats + d - 1, stat, statr.at[d - 1], at_cent(d))

    top = functools.reduce(jnp.maximum, [mtop[c] for c in range(n_chunk)])
    total = sum(msum[c] * jnp.exp2(mtop[c] - top) for c in range(n_chunk))
    for i in range(n_points // 128):
        stat[0, i : i + 1, :] = top[:, i * 128 : (i + 1) * 128]
        stat[1, i : i + 1, :] = total[:, i * 128 : (i + 1) * 128]
    for d in range(1, n_cent):
        stat_copy(d).start()
    sent.extend(stat_copy(d) for d in range(1, n_cent))

    def absorb():
        for d in range(1, n_cent):
            stat_copy(d).wait_recv()
        tops = [stat[0]] + [statr[d, 0] for d in range(n_cent - 1)]
        sums = [stat[1]] + [statr[d, 1] for d in range(n_cent - 1)]
        high = functools.reduce(jnp.maximum, tops)
        inverse = 1.0 / sum(s * jnp.exp2(t - high) for t, s in zip(tops, sums))
        for i in range(n_points // 128):
            row[0, :, i * 128 : (i + 1) * 128] = high[i : i + 1, :]
            row[1, :, i * 128 : (i + 1) * 128] = inverse[i : i + 1, :]
        for c in range(n_chunk):
            factor[c] = jnp.exp2(mtop[c] - row[0]) * row[1]

    us, vs = (slot, z), (z, slot)
    fins = []
    for c in range(2):
        for h in range(2):
            at = ((c * 4 + us[c]) * 2 + h) * (4 * rows) + vs[c] * rows
            fins.append(
                pltpu.make_async_copy(
                    cents.at[pl.ds(pl.multiple_of(at, rows), rows)],
                    cfin.at[c, h],
                    lsem.at[6 + 2 * c + h],
                )
            )
            fins[-1].start()

    def own_row(i):
        c = lax.div(i, 4)
        return (
            c,
            (1 - c) * ((4 * half + i) * 4 * rows)
            + c * (32 * rows + (i - 4) * 8 * rows + half * 2 * rows),
        )

    def gather(ref, i, cols):
        c, at = own_row(i)
        at = pl.multiple_of(at, 2 * rows)
        low = ref[pl.ds(at, 2 * rows), cols]
        at = pl.multiple_of(at + (1 + c) * 2 * rows, 2 * rows)
        return jnp.concatenate([low, ref[pl.ds(at, 2 * rows), cols]], axis=0)

    def add_up(count, resp):
        wide = resp.astype(F32)
        for l in range(tile // 128):
            count += wide[:, l * 128 : (l + 1) * 128]
        return count

    def put(i, acc, count, fresh):
        acc = acc.reshape(4, rows, width)
        w[i] = acc if fresh else w[i] + acc
        line = jnp.sum(count.T, axis=0, keepdims=True)
        for b in range(4):
            piece = line[:, b * rows : (b + 1) * rows]
            cnt[i, b, :, :rows] = piece if fresh else cnt[i, b, :, :rows] + piece

    def with_own(i, carry):
        group = lax.div(own_row(i)[1], chunk)
        acc = jnp.zeros((4 * rows, width), F32)
        count = jnp.zeros((4 * rows, 128), F32)
        for t in range(n_tile):
            cols = slice(t * tile, (t + 1) * tile)
            resp = (gather(expo, i, cols).astype(F32) * factor[group, :, cols]).astype(BF16)
            acc += jnp.dot(resp, ph[cols, :], preferred_element_type=F32)
            count = add_up(count, resp)
        put(i, acc, count, True)
        return carry

    everything = slice(None)

    def with_other(i, steps):
        acc = jnp.zeros((4 * rows, width), F32)
        count = jnp.zeros((4 * rows, 128), F32)
        cent = gather(ch, i, everything)
        square = jnp.concatenate([gather(sqb, i, everything)] * (tile // 128), axis=1)
        for d in steps:
            cols = pl.ds(pl.multiple_of(lax.rem(y + d, 4) * tile, tile), tile)
            inner = lax.dot_general(
                cent, pho[cols, :], (((1,), (1,)), ((), ())), preferred_element_type=F32
            )
            value = inner * (2.0 * scale) - square - rowo[0, :, cols]
            resp = (jnp.exp2(value) * rowo[1, :, cols]).astype(BF16)
            acc += jnp.dot(resp, pho[cols, :], preferred_element_type=F32)
            count = add_up(count, resp)
        put(i, acc, count, False)

    def round_other(d):
        for i in range(4):
            side_copy(d, i).wait_recv()
        at = lax.rem(y + d, 4)
        value = pin[pl.ds(2 * at, 2)].reshape(tile, width)
        pho[pl.ds(pl.multiple_of(at * tile, tile), tile), :] = value.astype(BF16)

    relay(2)
    relay_next(0)
    relay(3)
    relay_next(1)
    absorb()
    rows_copy = send(row, rowo, friend)
    for i in range(4):
        bring_copy(i).wait_send()
    lax.fori_loop(0, 2, with_own, 0)
    relay_next(2)
    relay_far(2)
    lax.fori_loop(2, 4, with_own, 0)
    relay_far(0)
    relay_far(1)
    relay_far(3)
    lax.fori_loop(4, 8, with_own, 0)
    relay_next(3)
    rows_copy.wait_recv()

    ups = (at_x(1), at_z(1))
    downs = (at_x(3), at_z(3))
    xs = [slot_of(lax.rem(x + d, 4)) for d in range(4)]
    zs = [lax.rem(z + d, 4) for d in range(4)]
    u, v = (xs, zs), (zs, xs)
    order = (2, 1, 3, 0)
    theirs, mine = 1 - g, g

    def to_mate(h):
        for d in order:
            over[h, d] = send(w.at[theirs * 2 + h, zs[d]], x1.at[h, zs[d]], mate)

    over = {}
    early = (0, 1, 3)
    for d in early:
        round_other(d)
    with_other(theirs * 2, early)
    with_other(4 + zs[2], early)
    round_other(2)
    with_other(theirs * 2, (2,))
    to_mate(0)
    with_other(4 + zs[2], (2,))
    a_up = send(w.at[4 + zs[2], pl.ds(0, 2)], r1.at[0], ups[1])
    a_dn = send(w.at[4 + zs[2], pl.ds(2, 2)], r1.at[1], downs[1])
    with_other(theirs * 2 + 1, range(4))
    to_mate(1)
    with_other(4 + zs[1], range(4))
    n_up = send(w.at[4 + zs[1], pl.ds(2, 2)], r2.at[0, 1], ups[1])
    with_other(4 + zs[3], range(4))
    n_dn = send(w.at[4 + zs[3], pl.ds(0, 2)], r2.at[1, 0], downs[1])

    def rest(i, carry):
        top = lax.div(3 - i, 3)
        with_other(top * (4 + z) + (1 - top) * (mine * 2 + i - 1), range(4))
        return carry

    lax.fori_loop(0, 3, rest, 0)

    a_up.wait_recv()
    b_up, b_dn = [], []
    sides = (theirs, mine)
    for k in sides:
        w[4 + zs[1], k] += r1[0, k]
        b_up.append(send(w.at[4 + zs[1], k], r2.at[0, 0, k], ups[1]))
    a_dn.wait_recv()
    for k in sides:
        w[4 + zs[3], 2 + k] += r1[1, k]
        b_dn.append(send(w.at[4 + zs[3], 2 + k], r2.at[1, 1, k], downs[1]))

    copies = [send(cnt.at[pl.ds(theirs * 2, 2)], cx0, mate)]
    for h in range(2):
        copies.append(send(cnt.at[pl.ds(4, 4), 2 * h + theirs], cx1.at[h], mate))
    for copy in copies:
        copy.wait_recv()
    block = pl.ds(2 * mine, 2)
    cnt[block] = cnt[block] + cx0[...]
    for h in range(2):
        cnt[4:8, 2 * h + mine] = cnt[4:8, 2 * h + mine] + cx1[h]
    copies = []
    for d in (1, 2, 3):
        copies.append(send(cnt.at[block, zs[d]], cntz.at[0, d - 1], at_z(d)))
        for h in range(2):
            copies.append(
                send(cnt.at[4 + zs[d], 2 * h + mine], cntz.at[1, d - 1, h], at_z(d))
            )

    halves = [pl.ds(q * (rows // 2), rows // 2) for q in range(2)]
    s_up, s_dn, ends = {}, {}, ([], [])

    def pass_on(h, d, q):
        lane = h if d is None else 1 - h
        to = (ups[1], downs[1])[lane]
        b = zs[d or (1 + 2 * h)]
        ends[q].append(
            send(w.at[mine * 2 + h, b, halves[q]], t2.at[lane, h, halves[q]], to)
        )

    def settle(k, n):
        b_up[n].wait_recv()
        b_dn[n].wait_recv()
        for h in range(2):
            w[4 + z, 2 * h + k] += r2[0, h, k] + r2[1, h, k]

    last = []
    for d in order:
        for h in range(2):
            over[h, d].wait_recv()
            w[mine * 2 + h, zs[d]] += x1[h, zs[d]]
        if d == 2:
            for q in range(2):
                part = halves[q]
                s_up[q] = send(w.at[mine * 2, zs[2], part], t1.at[0, part], ups[1])
                s_dn[q] = send(w.at[mine * 2 + 1, zs[2], part], t1.at[1, part], downs[1])
            n_up.wait_recv()
            n_dn.wait_recv()
            settle(theirs, 0)
            for h in range(2):
                last.append(send(w.at[4 + z, 2 * h + theirs], x2.at[h], mate))
        if d == 1:
            pass_on(1, 1, 0)
        if d == 3:
            pass_on(0, 3, 0)
            settle(mine, 1)
    for q in range(2):
        if q == 1:
            pass_on(1, 1, 1)
            pass_on(0, 3, 1)
        part = halves[q]
        s_up[q].wait_recv()
        w[mine * 2, zs[1], part] += t1[0, part]
        pass_on(0, None, q)
        s_dn[q].wait_recv()
        w[mine * 2 + 1, zs[3], part] += t1[1, part]
        pass_on(1, None, q)

    for copy in copies:
        copy.wait_recv()
    for copy in fins:
        copy.wait()
    g_up, g_dn, h_up, h_dn, f_up, f_dn = {}, {}, {}, {}, {}, {}
    for c in range(2):
        counts = []
        for h in range(2):
            line = cnt[mine * 2 + h, z] if c == 0 else cnt[4 + z, 2 * h + mine]
            line = line + cntz[c, 0, h] + cntz[c, 1, h] + cntz[c, 2, h]
            counts.append(jnp.broadcast_to(line, (128, 128)).T + 1.0)
        for q in range(2):
            part = halves[q]
            if c == 0 or q == 0:
                for copy in last if c else ends[q]:
                    copy.wait_recv()
            for h in range(2):
                count = counts[h][q * (rows // 2) : (q + 1) * (rows // 2)]
                count = jnp.concatenate([count] * (width // 128), axis=1)
                if c == 0:
                    value = w[mine * 2 + h, z, part] + t2[0, h, part] + t2[1, h, part]
                else:
                    value = w[4 + z, 2 * h + mine, part] + x2[h, part]
                got[c, us[c], h, vs[c], part] = (value + cfin[c, h, part]) / count
            piece = got.at[c, us[c], :, vs[c], part]
            g_up[c, q] = send(piece, piece, ups[1 - c])
            g_dn[c, q] = send(piece, piece, downs[1 - c])
            h_up[c, q] = send(piece, piece, ups[c])
            h_dn[c, q] = send(piece, piece, downs[c])

    e_up, e_dn = {}, {}

    def spread(c, d):
        piece = got.at[c, us[c], :, v[c][d]]
        e_up[c, d] = send(piece, piece, ups[c])
        e_dn[c, d] = send(piece, piece, downs[c])

    for c in range(2):
        me = us[c]
        g_up[c, 0].wait_recv()
        g_up[c, 1].wait_recv()
        piece = got.at[c, me, 0, v[c][3]]
        f_up[c] = send(piece, piece, ups[1 - c])
        spread(c, 3)
        g_dn[c, 0].wait_recv()
        g_dn[c, 1].wait_recv()
        piece = got.at[c, me, 1, v[c][1]]
        f_dn[c] = send(piece, piece, downs[1 - c])
        spread(c, 1)
    k_up, k_dn = {}, {}

    def onward(c, d):
        b = v[c][d]
        for copy in [h_up[c, 0], h_up[c, 1]] if d == 0 else [e_up[c, d]]:
            copy.wait_recv()
        piece = got.at[c, u[c][3], 0, b]
        k_up[c, d] = send(piece, piece, ups[c])
        for copy in [h_dn[c, 0], h_dn[c, 1]] if d == 0 else [e_dn[c, d]]:
            copy.wait_recv()
        piece = got.at[c, u[c][1], 1, b]
        k_dn[c, d] = send(piece, piece, downs[c])

    for c in range(2):
        onward(c, 0)
    for c in range(2):
        f_up[c].wait_recv()
        f_dn[c].wait_recv()
        spread(c, 2)
    for d in (3, 1, 2):
        for c in range(2):
            onward(c, d)
    for d in (0, 3, 1, 2):
        for c in range(2):
            k_up[c, d].wait_recv()
            k_dn[c, d].wait_recv()
    for copy in sent:
        copy.wait_send()


def store(got, out, sem):
    copies = [
        pltpu.make_async_copy(got.at[c, pl.ds(2 * h, 2)], out.at[c, pl.ds(2 * h, 2)], sem.at[2 * c + h])
        for c in range(2)
        for h in range(2)
    ]
    for copy in copies:
        copy.start()
    for copy in copies:
        copy.wait()


def body(points, centroids):
    n_points, width = points.shape
    n_rows = centroids.shape[0]
    n_cent = lax.axis_size("cent")
    chunk, tile = n_rows // 4, 512
    rows = n_rows // 64
    pieces = (2, 4, 2, 4, rows, width)
    n_copies = 32 + (n_cent - 1) + 1 + 8 + 4 + 4 + 12 + 12 + 2 + 48
    vm = pltpu.VMEM
    flat = (n_rows // chunk, 1, n_points)
    piece = (rows, width)
    lines = (4, 1, 128)
    scratch = [
        vm((n_points, width), BF16),
        vm((n_points, width), BF16),
        vm((8, 4, *piece), F32),
        vm((2, chunk, width), F32),
        vm((n_rows, width), BF16),
        vm((n_rows, 128), F32),
        vm((chunk, tile), F32),
        vm((chunk, tile), F32),
        vm((n_rows, n_points), BF16),
        vm(flat, F32),
        vm(flat, F32),
        vm(flat, F32),
        vm((2, n_points // 128, 128), F32),
        vm((n_cent - 1, 2, n_points // 128, 128), F32),
        vm((2, 1, n_points), F32),
        vm((2, 1, n_points), F32),
        vm((8, 4, *piece), F32),
        vm((2, 4, *piece), F32),
        vm((2, *piece), F32),
        vm((2, 2, *piece), F32),
        vm((2, 2, 2, *piece), F32),
        vm((2, *piece), F32),
        vm((2, 2, *piece), F32),
        vm((2, 2, *piece), F32),
        vm((8, *lines), F32),
        vm((2, *lines), F32),
        vm((2, *lines), F32),
        vm((2, 3, 2, 1, 128), F32),
        pltpu.SemaphoreType.DMA((n_copies,)),
        pltpu.SemaphoreType.DMA((n_copies,)),
        pltpu.SemaphoreType.DMA((10,)),
    ]
    result = pl.pallas_call(
        functools.partial(kernel, n_cent),
        out_shape=pltpu.VMEM(pieces, F32),
        in_specs=[pl.BlockSpec(memory_space=pl.ANY)] * 2,
        out_specs=pl.BlockSpec(memory_space=pltpu.VMEM),
        scratch_shapes=scratch,
        compiler_params=pltpu.CompilerParams(
            collective_id=0, has_side_effects=True, vmem_limit_bytes=54 * 2**20
        ),
    )(points.reshape(8, 4, n_points // 32, width), centroids)
    saved = pl.pallas_call(
        store,
        out_shape=jax.ShapeDtypeStruct(pieces, F32),
        in_specs=[pl.BlockSpec(memory_space=pltpu.VMEM)],
        out_specs=pl.BlockSpec(memory_space=pl.ANY),
        scratch_shapes=[pltpu.SemaphoreType.DMA((4,))],
        compiler_params=pltpu.CompilerParams(vmem_limit_bytes=2**20),
    )(result)
    return saved.reshape(n_rows, width)


def solution(mesh):
    placed = (P("dp", None), P("cent", None))
    return jax.shard_map(
        body, mesh=mesh, in_specs=placed, out_specs=P("cent", None), check_vma=False
    )
```

```python
import functools

import jax
import jax.numpy as jnp
from jax import lax
from jax.experimental import pallas as pl
from jax.experimental.pallas import tpu as pltpu
from jax.sharding import PartitionSpec as P

MESH = pl.DeviceIdType.MESH
F32, BF16 = jnp.float32, jnp.bfloat16
LOG2E = 1.4426950408889634


def kernel(
    n_cent,
    points,
    cents,
    got,
    ph,
    cstage,
    ch,
    sqb,
    logit0,
    logit1,
    expo,
    mtop,
    msum,
    factor,
    stat,
    statr,
    row,
    w,
    r1,
    r2,
    t1,
    t2,
    cfin,
    cnt,
    cntx0,
    cntx1,
    cntz,
    ssem,
    rsem,
    lsem,
):
    n_points, width = ph.shape
    chunk = ch.shape[1]
    n_chunk = mtop.shape[0]
    tile = logit0.shape[1]
    n_tile = n_points // tile
    rows = w.shape[4]
    scale = LOG2E / width**0.5

    dp = lax.axis_index("dp")
    ce = lax.axis_index("cent")
    x, z = lax.rem(dp, 4), lax.div(dp, 4)

    def at_x(d):
        return (z * 4 + lax.rem(x + d, 4), ce)

    def at_z(d):
        return (lax.rem(z + d, 4) * 4 + x, ce)

    def at_cent(d):
        return (dp, lax.rem(ce + d, n_cent))

    peers = [at_x(d) for d in (1, 2, 3)] + [at_z(d) for d in (1, 2, 3)]
    peers += [at_cent(d) for d in range(1, n_cent)]
    barrier = pltpu.get_barrier_semaphore()
    for peer in peers:
        pl.semaphore_signal(barrier, inc=1, device_id=peer, device_id_type=MESH)

    used = [0]

    def slots(n):
        used[0] += n
        return used[0] - n

    def remote(i, src, dst, dev, s=0):
        return pltpu.make_async_remote_copy(
            src_ref=src,
            dst_ref=dst,
            send_sem=ssem.at[s],
            recv_sem=rsem.at[i],
            device_id=dev,
            device_id_type=MESH,
        )

    def send(i, src, dst, dev, s=0):
        remote(i, src, dst, dev, s).start()

    def wait(sem, ref):
        pltpu.make_async_copy(ref, ref, sem).wait()

    part = n_points // 4

    def load_points(i):
        return pltpu.make_async_copy(
            points.at[i], w.at[0, i], lsem.at[i]
        )

    def load_cents(i):
        slot = lax.rem(i, 2)
        return pltpu.make_async_copy(
            cents.at[pl.ds(i * chunk, chunk)], cstage.at[slot], lsem.at[4 + slot]
        )

    load_points(0).start()
    load_cents(0).start()
    for i in range(1, 4):
        load_points(i).start()
    load_cents(1).start()

    def round_cents(i):
        slot = lax.rem(i, 2)
        value = cstage[slot]
        ch[slot] = value.astype(BF16)
        sqb[slot] = jnp.broadcast_to(
            jnp.sum(value * value, axis=1, keepdims=True) * scale, (chunk, 128)
        )

    def first(c, t, logit):
        slot = lax.rem(c, 2)
        inner = lax.dot_general(
            ch[slot], ph[t * tile : (t + 1) * tile, :], (((1,), (1,)), ((), ())),
            preferred_element_type=F32,
        )
        value = inner * (2.0 * scale) - jnp.concatenate([sqb[slot]] * (tile // 128), axis=1)
        logit[...] = value
        return jnp.max(value, axis=0, keepdims=True)

    def second(c, t, logit, high):
        at = slice(t * tile, (t + 1) * tile)
        e = jnp.exp2(logit[...] - high)
        base = pl.multiple_of(c * chunk, chunk)
        expo[pl.ds(base, chunk), at] = e.astype(BF16)
        mtop[c, :, at] = high
        msum[c, :, at] = jnp.sum(e, axis=0, keepdims=True)

    logits = (logit0, logit1)

    def on_chunk(c, high, last):
        if not last:
            load_cents(c + 1).wait()

            @pl.when(c + 2 < n_chunk)
            def _():
                load_cents(c + 2).start()

        for t in range(n_tile):
            if t + 1 < n_tile:
                after = first(c, t + 1, logits[(t + 1) % 2])
                if t == 0 and not last:
                    round_cents(c + 1)
            elif not last:
                after = first(c + 1, 0, logits[(t + 1) % 2])
            second(c, t, logits[t % 2], high)
            high = after
        return high

    def round_points(i):
        load_points(i).wait()
        ph[i * part : (i + 1) * part, :] = w[0, i].reshape(part, width).astype(BF16)

    round_points(0)
    load_cents(0).wait()
    round_cents(0)
    high = first(0, 0, logit0)
    for i in range(1, 4):
        round_points(i)
    high = lax.fori_loop(0, n_chunk - 1, lambda c, high: on_chunk(c, high, False), high)
    on_chunk(n_chunk - 1, high, True)

    stats = slots(1)
    top = functools.reduce(jnp.maximum, [mtop[c] for c in range(n_chunk)])
    total = sum(msum[c] * jnp.exp2(mtop[c] - top) for c in range(n_chunk))
    for i in range(n_points // 128):
        stat[0, i : i + 1, :] = top[:, i * 128 : (i + 1) * 128]
        stat[1, i : i + 1, :] = total[:, i * 128 : (i + 1) * 128]
    pl.semaphore_wait(barrier, len(peers))
    for d in range(1, n_cent):
        send(stats, stat, statr.at[d - 1], at_cent(d), 1)

    def absorb():
        wait(rsem.at[stats], statr)
        tops = [stat[0]] + [statr[d, 0] for d in range(n_cent - 1)]
        sums = [stat[1]] + [statr[d, 1] for d in range(n_cent - 1)]
        high = functools.reduce(jnp.maximum, tops)
        inverse = 1.0 / sum(s * jnp.exp2(t - high) for t, s in zip(tops, sums))
        for i in range(n_points // 128):
            row[0, :, i * 128 : (i + 1) * 128] = high[i : i + 1, :]
            row[1, :, i * 128 : (i + 1) * 128] = inverse[i : i + 1, :]
        for c in range(n_chunk):
            factor[c] = jnp.exp2(mtop[c] - row[0]) * row[1]

    us, vs = (x, z), (z, x)
    fins = []
    for c in range(2):
        for h in range(2):
            at = ((c * 4 + us[c]) * 2 + h) * (4 * rows) + vs[c] * rows
            fins.append(
                pltpu.make_async_copy(
                    cents.at[pl.ds(pl.multiple_of(at, rows), rows)],
                    cfin.at[c, h],
                    lsem.at[6 + 2 * c + h],
                )
            )
            fins[-1].start()

    def produce(pieces):
        spots = []
        for block, b in pieces:
            at = block * (4 * rows) + (0 if b is None else b * rows)
            spots.append((pl.multiple_of(at, rows), lax.div(block * (4 * rows), chunk)))
        size = 4 * rows // len(pieces)
        acc = jnp.zeros((4 * rows, width), F32)
        count = jnp.zeros((4 * rows, 128), F32)
        for t in range(n_tile):
            cols = slice(t * tile, (t + 1) * tile)
            parts = [
                (expo[pl.ds(at, size), cols].astype(F32) * factor[group, :, cols]).astype(BF16)
                for at, group in spots
            ]
            resp = parts[0] if len(parts) == 1 else jnp.concatenate(parts, axis=0)
            acc += jnp.dot(resp, ph[cols, :], preferred_element_type=F32)
            wide = resp.astype(F32)
            for l in range(tile // 128):
                count += wide[:, l * 128 : (l + 1) * 128]
        line = jnp.sum(count.T, axis=0, keepdims=True)
        for k in range(4):
            block, b = pieces[k] if len(pieces) == 4 else (pieces[0][0], k)
            w[lax.div(block, 8), lax.rem(lax.div(block, 2), 4), lax.rem(block, 2), b] = acc[
                k * rows : (k + 1) * rows
            ]
            cnt[block, b, :, :rows] = line[:, k * rows : (k + 1) * rows]

    def block_of(c, bu, h):
        return (c * 4 + bu) * 2 + h

    ups = (at_x(1), at_z(1))
    downs = (at_x(3), at_z(3))
    u = [[lax.rem(us[c] + d, 4) for d in range(4)] for c in range(2)]
    v = [[lax.rem(vs[c] + d, 4) for d in range(4)] for c in range(2)]
    order = (2, 1, 3, 0)

    def place(c):
        return x * (1 - c) + z * c, z * (1 - c) + x * c

    def along(c, d):
        return (lax.rem(z + c * d, 4) * 4 + lax.rem(x + (1 - c) * d, 4), ce)

    far, near = slots(8), slots(1)

    def far_copy(c, h, k):
        here, other = place(c)
        step = lax.rem(2 + 3 * k + lax.div(k, 2) * 3 + lax.div(k, 3) * 2, 4)
        b = lax.rem(other + step, 4)
        return remote(
            far + c * 4 + k,
            w.at[c, lax.rem(here + 2, 4), h, b],
            r1.at[c, h, b],
            along(c, 1 + 2 * h),
        )

    def near_copy(c, h):
        here, _ = place(c)
        d = 3 - 2 * h
        return remote(
            near, w.at[c, lax.rem(here + d, 4), h], r2.at[c, 1 - h, h], along(c, d)
        )

    def farthest(k, carry):
        step = lax.rem(2 + 3 * k + lax.div(k, 2) * 3 + lax.div(k, 3) * 2, 4)
        produce(
            [
                (block_of(c, lax.rem(place(c)[0] + 2, 4), h), lax.rem(place(c)[1] + step, 4))
                for h in range(2)
                for c in range(2)
            ]
        )
        for h in range(2):
            for c in range(2):
                far_copy(c, h, k).start()
        return carry

    def nearest(i, carry):
        c, h = lax.rem(i, 2), 1 - lax.div(i, 2)
        produce([(block_of(c, lax.rem(place(c)[0] + 3 - 2 * h, 4), h), None)])
        near_copy(c, h).start()
        return carry

    def others(i, carry):
        c, h, mine = lax.rem(i, 2), lax.rem(lax.div(i, 2), 2), lax.div(i, 4)
        produce([(block_of(c, lax.rem(place(c)[0] + (1 - mine) * (1 + 2 * h), 4), h), None)])
        return carry

    absorb()
    lax.fori_loop(0, 4, farthest, 0)
    lax.fori_loop(0, 4, nearest, 0)
    lax.fori_loop(0, 8, others, 0)
    xrec = slots(2)
    for d in (1, 2, 3):
        to = lax.rem(x + d, 4)
        send(xrec, cnt.at[pl.ds(2 * to, 2)], cntx0.at[d - 1], at_x(d), 2)
        send(xrec + 1, cnt.at[pl.ds(8, 8), to], cntx1.at[d - 1], at_x(d), 3)

    two, four = w.at[0, 0, 0, pl.ds(0, 2)], w.at[0, 0, 0]
    tail = slots(8)
    for k, d in enumerate(order):
        for c in range(2):
            b = v[c][d]
            wait(rsem.at[far + c * 4 + k], two)
            at = tail + c * 4 + k
            w[c, u[c][1], 0, b] += r1[c, 0, b]
            send(at, w.at[c, u[c][1], 0, b], r2.at[c, 0, 0, b], ups[c])
            w[c, u[c][3], 1, b] += r1[c, 1, b]
            send(at, w.at[c, u[c][3], 1, b], r2.at[c, 1, 1, b], downs[c])
    wait(rsem.at[xrec], cntx0)
    wait(rsem.at[xrec + 1], cntx1)
    mine = pl.ds(2 * x, 2)
    cnt[mine] = cnt[mine] + cntx0[0] + cntx0[1] + cntx0[2]
    cnt[8:16, x] = cnt[8:16, x] + cntx1[0] + cntx1[1] + cntx1[2]
    zrec = slots(1)
    for d in (1, 2, 3):
        to = lax.rem(z + d, 4)
        send(zrec, cnt.at[mine, to], cntz.at[0, d - 1], at_z(d), 4)
        send(zrec, cnt.at[pl.ds(8 + 2 * to, 2), x], cntz.at[1, d - 1], at_z(d), 4)
    wait(rsem.at[near], w.at[0, pl.ds(0, 2)])

    ups2, downs2 = ups[::-1], downs[::-1]
    halves = [pl.ds(q * (rows // 2), rows // 2) for q in range(2)]
    early, ends = slots(4), slots(2)

    def pass_on(c, h, d, q):
        side = h if d is None else 1 - h
        to = (ups2, downs2)[side][c]
        b = v[c][d or (1 + 2 * h)]
        send(
            ends + q, w.at[c, us[c], h, b, halves[q]], t2.at[c, side, h, halves[q]], to
        )

    for k, d in enumerate(order):
        for c in range(2):
            b, me = v[c][d], us[c]
            wait(rsem.at[tail + c * 4 + k], two)
            for h in range(2):
                w[c, me, h, b] += r2[c, 0, h, b] + r2[c, 1, h, b]
            if d == 2:
                for q in range(2):
                    part, at = halves[q], early + 2 * c + q
                    send(at, w.at[c, me, 0, b, part], t1.at[c, 0, part], ups2[c])
                    send(at, w.at[c, me, 1, b, part], t1.at[c, 1, part], downs2[c])
            if d == 1:
                pass_on(c, 1, 1, 0)
            if d == 3:
                pass_on(c, 0, 3, 0)
    for q in range(2):
        if q == 1:
            for c in range(2):
                pass_on(c, 1, 1, 1)
                pass_on(c, 0, 3, 1)
        for c in range(2):
            me, part = us[c], halves[q]
            wait(rsem.at[early + 2 * c + q], w.at[0, 0, 0, 0])
            w[c, me, 0, v[c][1], part] += t1[c, 0, part]
            pass_on(c, 0, None, q)
            w[c, me, 1, v[c][3], part] += t1[c, 1, part]
            pass_on(c, 1, None, q)

    wait(rsem.at[zrec], cntz)
    for copy in fins:
        copy.wait()
    counts = {}
    for c in range(2):
        for h in range(2):
            line = cnt[(c * 4 + us[c]) * 2 + h, vs[c]]
            line = line + cntz[c, 0, h] + cntz[c, 1, h] + cntz[c, 2, h]
            counts[c, h] = jnp.broadcast_to(line, (128, 128)).T + 1.0
    g, h_, f, e, k_ = slots(4), slots(2), slots(2), slots(6), slots(1)
    for q in range(2):
        wait(rsem.at[ends + q], four)
        part = halves[q]
        for c in range(2):
            me, b = us[c], vs[c]
            for h in range(2):
                count = counts[c, h][q * (rows // 2) : (q + 1) * (rows // 2)]
                count = jnp.concatenate([count] * (width // 128), axis=1)
                value = w[c, me, h, b, part] + t2[c, 0, h, part] + t2[c, 1, h, part]
                got[c, me, h, b, part] = (value + cfin[c, h, part]) / count
            piece = got.at[c, me, :, b, part]
            send(g + 2 * c, piece, piece, ups2[c])
            send(g + 2 * c + 1, piece, piece, downs2[c])
        for c in range(2):
            piece = got.at[c, us[c], :, vs[c], part]
            send(h_ + c, piece, piece, ups[c])
            send(h_ + c, piece, piece, downs[c])

    def spread(c, d):
        piece = got.at[c, us[c], :, v[c][d]]
        at = e + 3 * c + d - 1
        send(at, piece, piece, ups[c])
        send(at, piece, piece, downs[c])

    def onward(c, d):
        b = v[c][d]
        wait(rsem.at[h_ + c if d == 0 else e + 3 * c + d - 1], four)
        piece = got.at[c, u[c][3], 0, b]
        send(k_, piece, piece, ups[c])
        piece = got.at[c, u[c][1], 1, b]
        send(k_, piece, piece, downs[c])

    for c in range(2):
        wait(rsem.at[g + 2 * c], two)
        piece = got.at[c, us[c], 0, v[c][3]]
        send(f + c, piece, piece, ups2[c])
        spread(c, 3)
        wait(rsem.at[g + 2 * c + 1], two)
        piece = got.at[c, us[c], 1, v[c][1]]
        send(f + c, piece, piece, downs2[c])
        spread(c, 1)
    for c in range(2):
        onward(c, 0)
    for c in range(2):
        wait(rsem.at[f + c], two)
        spread(c, 2)
    for d in (3, 1, 2):
        for c in range(2):
            onward(c, d)
    wait(rsem.at[k_], w.at[0, pl.ds(0, 2)])
    total_rows = expo.shape[0] * 15 // 16
    wait(ssem.at[0], expo.at[pl.ds(0, total_rows)])
    wait(ssem.at[1], statr)
    wait(ssem.at[2], cntx0)
    wait(ssem.at[3], cntx1)
    wait(ssem.at[4], cntz)


def store(got, out, sem):
    copies = [
        pltpu.make_async_copy(got.at[c, pl.ds(2 * h, 2)], out.at[c, pl.ds(2 * h, 2)], sem.at[2 * c + h])
        for c in range(2)
        for h in range(2)
    ]
    for copy in copies:
        copy.start()
    for copy in copies:
        copy.wait()


def body(points, centroids):
    n_points, width = points.shape
    n_rows = centroids.shape[0]
    n_cent = lax.axis_size("cent")
    chunk, tile = n_rows // 4, 512
    rows = n_rows // 64
    pieces = (2, 4, 2, 4, rows, width)
    n_groups = 1 + 9 + 2 + 8 + 1 + 6 + 15
    vm = pltpu.VMEM
    flat = (n_rows // chunk, 1, n_points)
    scratch = [
        vm((n_points, width), BF16),
        vm((2, chunk, width), F32),
        vm((2, chunk, width), BF16),
        vm((2, chunk, 128), F32),
        vm((chunk, tile), F32),
        vm((chunk, tile), F32),
        vm((n_rows, n_points), BF16),
        vm(flat, F32),
        vm(flat, F32),
        vm(flat, F32),
        vm((2, n_points // 128, 128), F32),
        vm((n_cent - 1, 2, n_points // 128, 128), F32),
        vm((2, 1, n_points), F32),
        vm(pieces, F32),
        vm((2, 2, 4, rows, width), F32),
        vm((2, 2, 2, 4, rows, width), F32),
        vm((2, 2, rows, width), F32),
        vm((2, 2, 2, rows, width), F32),
        vm((2, 2, rows, width), F32),
        vm((16, 4, 1, 128), F32),
        vm((3, 2, 4, 1, 128), F32),
        vm((3, 8, 1, 128), F32),
        vm((2, 3, 2, 1, 128), F32),
        pltpu.SemaphoreType.DMA((5,)),
        pltpu.SemaphoreType.DMA((n_groups,)),
        pltpu.SemaphoreType.DMA((10,)),
    ]
    result = pl.pallas_call(
        functools.partial(kernel, n_cent),
        out_shape=pltpu.VMEM(pieces, F32),
        in_specs=[pl.BlockSpec(memory_space=pl.ANY)] * 2,
        out_specs=pl.BlockSpec(memory_space=pltpu.VMEM),
        scratch_shapes=scratch,
        compiler_params=pltpu.CompilerParams(
            collective_id=0, has_side_effects=True, vmem_limit_bytes=54 * 2**20
        ),
    )(points.reshape(4, 2, 4, n_points // 32, width), centroids)
    saved = pl.pallas_call(
        store,
        out_shape=jax.ShapeDtypeStruct(pieces, F32),
        in_specs=[pl.BlockSpec(memory_space=pltpu.VMEM)],
        out_specs=pl.BlockSpec(memory_space=pl.ANY),
        scratch_shapes=[pltpu.SemaphoreType.DMA((4,))],
        compiler_params=pltpu.CompilerParams(vmem_limit_bytes=2**20),
    )(result)
    return saved.reshape(n_rows, width)


def solution(mesh):
    placed = (P("dp", None), P("cent", None))
    return jax.shard_map(
        body, mesh=mesh, in_specs=placed, out_specs=P("cent", None), check_vma=False
    )
```

```python
import functools

import jax
import jax.numpy as jnp
from jax import lax
from jax.experimental import pallas as pl
from jax.experimental.pallas import tpu as pltpu
from jax.sharding import PartitionSpec as P

MESH = pl.DeviceIdType.MESH
F32, BF16 = jnp.float32, jnp.bfloat16
LOG2E = 1.4426950408889634


def kernel(
    n_cent,
    points,
    cents,
    got,
    ph,
    pt,
    cstage,
    ch,
    sqb,
    logit0,
    logit1,
    expo,
    mtop,
    msum,
    factor,
    stat,
    statr,
    row,
    w,
    r1,
    r2,
    t1,
    t2,
    cfin,
    cnt,
    cntx0,
    cntx1,
    cntz,
    ssem,
    rsem,
    lsem,
):
    n_points, width = ph.shape
    chunk = ch.shape[1]
    n_chunk = mtop.shape[0]
    tile = logit0.shape[1]
    n_tile = n_points // tile
    rows = w.shape[4]
    scale = LOG2E / width**0.5

    dp = lax.axis_index("dp")
    ce = lax.axis_index("cent")
    x, z = lax.rem(dp, 4), lax.div(dp, 4)

    def at_x(d):
        return (z * 4 + lax.rem(x + d, 4), ce)

    def at_z(d):
        return (lax.rem(z + d, 4) * 4 + x, ce)

    def at_cent(d):
        return (dp, lax.rem(ce + d, n_cent))

    peers = [at_x(d) for d in (1, 2, 3)] + [at_z(d) for d in (1, 2, 3)]
    peers += [at_cent(d) for d in range(1, n_cent)]
    barrier = pltpu.get_barrier_semaphore()
    for peer in peers:
        pl.semaphore_signal(barrier, inc=1, device_id=peer, device_id_type=MESH)

    used = [0]

    def slots(n):
        used[0] += n
        return used[0] - n

    def remote(i, src, dst, dev, s=0):
        return pltpu.make_async_remote_copy(
            src_ref=src,
            dst_ref=dst,
            send_sem=ssem.at[s],
            recv_sem=rsem.at[i],
            device_id=dev,
            device_id_type=MESH,
        )

    def send(i, src, dst, dev, s=0):
        remote(i, src, dst, dev, s).start()

    def wait(sem, ref):
        pltpu.make_async_copy(ref, ref, sem).wait()

    part = n_points // 4

    def load_points(i):
        return pltpu.make_async_copy(
            points.at[i], w.at[0, i], lsem.at[i]
        )

    def load_cents(i):
        slot = lax.rem(i, 2)
        return pltpu.make_async_copy(
            cents.at[pl.ds(i * chunk, chunk)], cstage.at[slot], lsem.at[4 + slot]
        )

    load_points(0).start()
    load_cents(0).start()
    for i in range(1, 4):
        load_points(i).start()
    load_cents(1).start()

    def round_cents(i):
        slot = lax.rem(i, 2)
        value = cstage[slot]
        ch[slot] = value.astype(BF16)
        sqb[slot] = jnp.broadcast_to(
            jnp.sum(value * value, axis=1, keepdims=True) * scale, (chunk, 128)
        )

    def first(c, t, logit):
        slot = lax.rem(c, 2)
        inner = lax.dot_general(
            ch[slot], pt[:, t * tile : (t + 1) * tile], (((1,), (0,)), ((), ())),
            preferred_element_type=F32,
        )
        value = inner * (2.0 * scale) - jnp.concatenate([sqb[slot]] * (tile // 128), axis=1)
        logit[...] = value
        return jnp.max(value, axis=0, keepdims=True)

    def second(c, t, logit, high):
        at = slice(t * tile, (t + 1) * tile)
        e = jnp.exp2(logit[...] - high)
        base = pl.multiple_of(c * chunk, chunk)
        expo[pl.ds(base, chunk), at] = e.astype(BF16)
        mtop[c, :, at] = high
        msum[c, :, at] = jnp.sum(e, axis=0, keepdims=True)

    logits = (logit0, logit1)

    def on_chunk(c, high, last):
        if not last:
            load_cents(c + 1).wait()

            @pl.when(c + 2 < n_chunk)
            def _():
                load_cents(c + 2).start()

        for t in range(n_tile):
            if t + 1 < n_tile:
                after = first(c, t + 1, logits[(t + 1) % 2])
                if t == 0 and not last:
                    round_cents(c + 1)
            elif not last:
                after = first(c + 1, 0, logits[(t + 1) % 2])
            second(c, t, logits[t % 2], high)
            high = after
        return high

    def round_points(i):
        load_points(i).wait()
        half = w[0, i].reshape(part, width).astype(BF16)
        ph[i * part : (i + 1) * part, :] = half
        pt[:, i * part : (i + 1) * part] = half.T

    round_points(0)
    load_cents(0).wait()
    round_cents(0)
    high = first(0, 0, logit0)
    for i in range(1, 4):
        round_points(i)
    high = lax.fori_loop(0, n_chunk - 1, lambda c, high: on_chunk(c, high, False), high)
    on_chunk(n_chunk - 1, high, True)

    stats = slots(1)
    top = functools.reduce(jnp.maximum, [mtop[c] for c in range(n_chunk)])
    total = sum(msum[c] * jnp.exp2(mtop[c] - top) for c in range(n_chunk))
    for i in range(n_points // 128):
        stat[0, i : i + 1, :] = top[:, i * 128 : (i + 1) * 128]
        stat[1, i : i + 1, :] = total[:, i * 128 : (i + 1) * 128]
    pl.semaphore_wait(barrier, len(peers))
    for d in range(1, n_cent):
        send(stats, stat, statr.at[d - 1], at_cent(d), 1)

    def absorb():
        wait(rsem.at[stats], statr)
        tops = [stat[0]] + [statr[d, 0] for d in range(n_cent - 1)]
        sums = [stat[1]] + [statr[d, 1] for d in range(n_cent - 1)]
        high = functools.reduce(jnp.maximum, tops)
        inverse = 1.0 / sum(s * jnp.exp2(t - high) for t, s in zip(tops, sums))
        for i in range(n_points // 128):
            row[0, :, i * 128 : (i + 1) * 128] = high[i : i + 1, :]
            row[1, :, i * 128 : (i + 1) * 128] = inverse[i : i + 1, :]
        for c in range(n_chunk):
            factor[c] = jnp.exp2(mtop[c] - row[0]) * row[1]

    us, vs = (x, z), (z, x)
    fins = []
    for c in range(2):
        for h in range(2):
            at = ((c * 4 + us[c]) * 2 + h) * (4 * rows) + vs[c] * rows
            fins.append(
                pltpu.make_async_copy(
                    cents.at[pl.ds(pl.multiple_of(at, rows), rows)],
                    cfin.at[c, h],
                    lsem.at[6 + 2 * c + h],
                )
            )
            fins[-1].start()

    def produce(pieces):
        spots = []
        for block, b in pieces:
            at = block * (4 * rows) + (0 if b is None else b * rows)
            spots.append((pl.multiple_of(at, rows), lax.div(block * (4 * rows), chunk)))
        size = 4 * rows // len(pieces)
        acc = jnp.zeros((4 * rows, width), F32)
        count = jnp.zeros((4 * rows, 128), F32)
        for t in range(n_tile):
            cols = slice(t * tile, (t + 1) * tile)
            parts = [
                (expo[pl.ds(at, size), cols].astype(F32) * factor[group, :, cols]).astype(BF16)
                for at, group in spots
            ]
            resp = parts[0] if len(parts) == 1 else jnp.concatenate(parts, axis=0)
            acc += jnp.dot(resp, ph[cols, :], preferred_element_type=F32)
            wide = resp.astype(F32)
            for l in range(tile // 128):
                count += wide[:, l * 128 : (l + 1) * 128]
        line = jnp.sum(count.T, axis=0, keepdims=True)
        for k in range(4):
            block, b = pieces[k] if len(pieces) == 4 else (pieces[0][0], k)
            w[lax.div(block, 8), lax.rem(lax.div(block, 2), 4), lax.rem(block, 2), b] = acc[
                k * rows : (k + 1) * rows
            ]
            cnt[block, b, :, :rows] = line[:, k * rows : (k + 1) * rows]

    def block_of(c, bu, h):
        return (c * 4 + bu) * 2 + h

    ups = (at_x(1), at_z(1))
    downs = (at_x(3), at_z(3))
    u = [[lax.rem(us[c] + d, 4) for d in range(4)] for c in range(2)]
    v = [[lax.rem(vs[c] + d, 4) for d in range(4)] for c in range(2)]
    order = (2, 1, 3, 0)

    def place(c):
        return x * (1 - c) + z * c, z * (1 - c) + x * c

    def along(c, d):
        return (lax.rem(z + c * d, 4) * 4 + lax.rem(x + (1 - c) * d, 4), ce)

    far, near = slots(8), slots(1)

    def far_copy(c, h, k):
        here, other = place(c)
        step = lax.rem(2 + 3 * k + lax.div(k, 2) * 3 + lax.div(k, 3) * 2, 4)
        b = lax.rem(other + step, 4)
        return remote(
            far + c * 4 + k,
            w.at[c, lax.rem(here + 2, 4), h, b],
            r1.at[c, h, b],
            along(c, 1 + 2 * h),
        )

    def near_copy(c, h):
        here, _ = place(c)
        d = 3 - 2 * h
        return remote(
            near, w.at[c, lax.rem(here + d, 4), h], r2.at[c, 1 - h, h], along(c, d)
        )

    def farthest(k, carry):
        step = lax.rem(2 + 3 * k + lax.div(k, 2) * 3 + lax.div(k, 3) * 2, 4)
        produce(
            [
                (block_of(c, lax.rem(place(c)[0] + 2, 4), h), lax.rem(place(c)[1] + step, 4))
                for h in range(2)
                for c in range(2)
            ]
        )
        for h in range(2):
            for c in range(2):
                far_copy(c, h, k).start()
        return carry

    def nearest(i, carry):
        c, h = lax.rem(i, 2), 1 - lax.div(i, 2)
        produce([(block_of(c, lax.rem(place(c)[0] + 3 - 2 * h, 4), h), None)])
        near_copy(c, h).start()
        return carry

    def others(i, carry):
        c, h, mine = lax.rem(i, 2), lax.rem(lax.div(i, 2), 2), lax.div(i, 4)
        produce([(block_of(c, lax.rem(place(c)[0] + (1 - mine) * (1 + 2 * h), 4), h), None)])
        return carry

    absorb()
    lax.fori_loop(0, 4, farthest, 0)
    lax.fori_loop(0, 4, nearest, 0)
    lax.fori_loop(0, 8, others, 0)
    xrec = slots(2)
    for d in (1, 2, 3):
        to = lax.rem(x + d, 4)
        send(xrec, cnt.at[pl.ds(2 * to, 2)], cntx0.at[d - 1], at_x(d), 2)
        send(xrec + 1, cnt.at[pl.ds(8, 8), to], cntx1.at[d - 1], at_x(d), 3)

    two, four = w.at[0, 0, 0, pl.ds(0, 2)], w.at[0, 0, 0]
    tail = slots(8)
    for k, d in enumerate(order):
        for c in range(2):
            b = v[c][d]
            wait(rsem.at[far + c * 4 + k], two)
            at = tail + c * 4 + k
            w[c, u[c][1], 0, b] += r1[c, 0, b]
            send(at, w.at[c, u[c][1], 0, b], r2.at[c, 0, 0, b], ups[c])
            w[c, u[c][3], 1, b] += r1[c, 1, b]
            send(at, w.at[c, u[c][3], 1, b], r2.at[c, 1, 1, b], downs[c])
    wait(rsem.at[xrec], cntx0)
    wait(rsem.at[xrec + 1], cntx1)
    mine = pl.ds(2 * x, 2)
    cnt[mine] = cnt[mine] + cntx0[0] + cntx0[1] + cntx0[2]
    cnt[8:16, x] = cnt[8:16, x] + cntx1[0] + cntx1[1] + cntx1[2]
    zrec = slots(1)
    for d in (1, 2, 3):
        to = lax.rem(z + d, 4)
        send(zrec, cnt.at[mine, to], cntz.at[0, d - 1], at_z(d), 4)
        send(zrec, cnt.at[pl.ds(8 + 2 * to, 2), x], cntz.at[1, d - 1], at_z(d), 4)
    wait(rsem.at[near], w.at[0, pl.ds(0, 2)])

    ups2, downs2 = ups[::-1], downs[::-1]
    halves = [pl.ds(q * (rows // 2), rows // 2) for q in range(2)]
    early, ends = slots(4), slots(2)

    def pass_on(c, h, d, q):
        side = h if d is None else 1 - h
        to = (ups2, downs2)[side][c]
        b = v[c][d or (1 + 2 * h)]
        send(
            ends + q, w.at[c, us[c], h, b, halves[q]], t2.at[c, side, h, halves[q]], to
        )

    for k, d in enumerate(order):
        for c in range(2):
            b, me = v[c][d], us[c]
            wait(rsem.at[tail + c * 4 + k], two)
            for h in range(2):
                w[c, me, h, b] += r2[c, 0, h, b] + r2[c, 1, h, b]
            if d == 2:
                for q in range(2):
                    part, at = halves[q], early + 2 * c + q
                    send(at, w.at[c, me, 0, b, part], t1.at[c, 0, part], ups2[c])
                    send(at, w.at[c, me, 1, b, part], t1.at[c, 1, part], downs2[c])
            if d == 1:
                pass_on(c, 1, 1, 0)
            if d == 3:
                pass_on(c, 0, 3, 0)
    for q in range(2):
        if q == 1:
            for c in range(2):
                pass_on(c, 1, 1, 1)
                pass_on(c, 0, 3, 1)
        for c in range(2):
            me, part = us[c], halves[q]
            wait(rsem.at[early + 2 * c + q], w.at[0, 0, 0, 0])
            w[c, me, 0, v[c][1], part] += t1[c, 0, part]
            pass_on(c, 0, None, q)
            w[c, me, 1, v[c][3], part] += t1[c, 1, part]
            pass_on(c, 1, None, q)

    wait(rsem.at[zrec], cntz)
    for copy in fins:
        copy.wait()
    counts = {}
    for c in range(2):
        for h in range(2):
            line = cnt[(c * 4 + us[c]) * 2 + h, vs[c]]
            line = line + cntz[c, 0, h] + cntz[c, 1, h] + cntz[c, 2, h]
            counts[c, h] = jnp.broadcast_to(line, (128, 128)).T + 1.0
    g, h_, f, e, k_ = slots(4), slots(2), slots(2), slots(6), slots(1)
    for q in range(2):
        wait(rsem.at[ends + q], four)
        part = halves[q]
        for c in range(2):
            me, b = us[c], vs[c]
            for h in range(2):
                count = counts[c, h][q * (rows // 2) : (q + 1) * (rows // 2)]
                count = jnp.concatenate([count] * (width // 128), axis=1)
                value = w[c, me, h, b, part] + t2[c, 0, h, part] + t2[c, 1, h, part]
                got[c, me, h, b, part] = (value + cfin[c, h, part]) / count
            piece = got.at[c, me, :, b, part]
            send(g + 2 * c, piece, piece, ups2[c])
            send(g + 2 * c + 1, piece, piece, downs2[c])
        for c in range(2):
            piece = got.at[c, us[c], :, vs[c], part]
            send(h_ + c, piece, piece, ups[c])
            send(h_ + c, piece, piece, downs[c])

    def spread(c, d):
        piece = got.at[c, us[c], :, v[c][d]]
        at = e + 3 * c + d - 1
        send(at, piece, piece, ups[c])
        send(at, piece, piece, downs[c])

    def onward(c, d):
        b = v[c][d]
        wait(rsem.at[h_ + c if d == 0 else e + 3 * c + d - 1], four)
        piece = got.at[c, u[c][3], 0, b]
        send(k_, piece, piece, ups[c])
        piece = got.at[c, u[c][1], 1, b]
        send(k_, piece, piece, downs[c])

    for c in range(2):
        wait(rsem.at[g + 2 * c], two)
        piece = got.at[c, us[c], 0, v[c][3]]
        send(f + c, piece, piece, ups2[c])
        spread(c, 3)
        wait(rsem.at[g + 2 * c + 1], two)
        piece = got.at[c, us[c], 1, v[c][1]]
        send(f + c, piece, piece, downs2[c])
        spread(c, 1)
    for c in range(2):
        onward(c, 0)
    for c in range(2):
        wait(rsem.at[f + c], two)
        spread(c, 2)
    for d in (3, 1, 2):
        for c in range(2):
            onward(c, d)
    wait(rsem.at[k_], w.at[0, pl.ds(0, 2)])
    total_rows = expo.shape[0] * 15 // 16
    wait(ssem.at[0], expo.at[pl.ds(0, total_rows)])
    wait(ssem.at[1], statr)
    wait(ssem.at[2], cntx0)
    wait(ssem.at[3], cntx1)
    wait(ssem.at[4], cntz)


def store(got, out, sem):
    copies = [
        pltpu.make_async_copy(got.at[c, pl.ds(2 * h, 2)], out.at[c, pl.ds(2 * h, 2)], sem.at[2 * c + h])
        for c in range(2)
        for h in range(2)
    ]
    for copy in copies:
        copy.start()
    for copy in copies:
        copy.wait()


def body(points, centroids):
    n_points, width = points.shape
    n_rows = centroids.shape[0]
    n_cent = lax.axis_size("cent")
    chunk, tile = n_rows // 4, 512
    rows = n_rows // 64
    pieces = (2, 4, 2, 4, rows, width)
    n_groups = 1 + 9 + 2 + 8 + 1 + 6 + 15
    vm = pltpu.VMEM
    flat = (n_rows // chunk, 1, n_points)
    scratch = [
        vm((n_points, width), BF16),
        vm((width, n_points), BF16),
        vm((2, chunk, width), F32),
        vm((2, chunk, width), BF16),
        vm((2, chunk, 128), F32),
        vm((chunk, tile), F32),
        vm((chunk, tile), F32),
        vm((n_rows, n_points), BF16),
        vm(flat, F32),
        vm(flat, F32),
        vm(flat, F32),
        vm((2, n_points // 128, 128), F32),
        vm((n_cent - 1, 2, n_points // 128, 128), F32),
        vm((2, 1, n_points), F32),
        vm(pieces, F32),
        vm((2, 2, 4, rows, width), F32),
        vm((2, 2, 2, 4, rows, width), F32),
        vm((2, 2, rows, width), F32),
        vm((2, 2, 2, rows, width), F32),
        vm((2, 2, rows, width), F32),
        vm((16, 4, 1, 128), F32),
        vm((3, 2, 4, 1, 128), F32),
        vm((3, 8, 1, 128), F32),
        vm((2, 3, 2, 1, 128), F32),
        pltpu.SemaphoreType.DMA((5,)),
        pltpu.SemaphoreType.DMA((n_groups,)),
        pltpu.SemaphoreType.DMA((10,)),
    ]
    result = pl.pallas_call(
        functools.partial(kernel, n_cent),
        out_shape=pltpu.VMEM(pieces, F32),
        in_specs=[pl.BlockSpec(memory_space=pl.ANY)] * 2,
        out_specs=pl.BlockSpec(memory_space=pltpu.VMEM),
        scratch_shapes=scratch,
        compiler_params=pltpu.CompilerParams(
            collective_id=0, has_side_effects=True, vmem_limit_bytes=55 * 2**20
        ),
    )(points.reshape(4, 2, 4, n_points // 32, width), centroids)
    saved = pl.pallas_call(
        store,
        out_shape=jax.ShapeDtypeStruct(pieces, F32),
        in_specs=[pl.BlockSpec(memory_space=pltpu.VMEM)],
        out_specs=pl.BlockSpec(memory_space=pl.ANY),
        scratch_shapes=[pltpu.SemaphoreType.DMA((4,))],
        compiler_params=pltpu.CompilerParams(vmem_limit_bytes=2**20),
    )(result)
    return saved.reshape(n_rows, width)


def solution(mesh):
    placed = (P("dp", None), P("cent", None))
    return jax.shard_map(
        body, mesh=mesh, in_specs=placed, out_specs=P("cent", None), check_vma=False
    )
```

```python
import functools

import jax
import jax.numpy as jnp
from jax import lax
from jax.experimental import pallas as pl
from jax.experimental.pallas import tpu as pltpu
from jax.sharding import PartitionSpec as P

MESH = pl.DeviceIdType.MESH
F32, BF16 = jnp.float32, jnp.bfloat16
LOG2E = 1.4426950408889634


def kernel(
    n_cent,
    points,
    cents,
    got,
    ph,
    pt,
    cstage,
    ch,
    sqb,
    logit0,
    logit1,
    expo,
    mtop,
    msum,
    factor,
    stat,
    statr,
    row,
    w,
    r1,
    r2,
    t1,
    t2,
    cfin,
    cnt,
    cntx0,
    cntx1,
    cntz,
    ssem,
    rsem,
    lsem,
):
    n_points, width = ph.shape
    chunk = ch.shape[1]
    n_chunk = mtop.shape[0]
    tile = logit0.shape[1]
    n_tile = n_points // tile
    rows = w.shape[4]
    scale = LOG2E / width**0.5

    dp = lax.axis_index("dp")
    ce = lax.axis_index("cent")
    x, z = lax.rem(dp, 4), lax.div(dp, 4)

    def at_x(d):
        return (z * 4 + lax.rem(x + d, 4), ce)

    def at_z(d):
        return (lax.rem(z + d, 4) * 4 + x, ce)

    def at_cent(d):
        return (dp, lax.rem(ce + d, n_cent))

    peers = [at_x(d) for d in (1, 2, 3)] + [at_z(d) for d in (1, 2, 3)]
    peers += [at_cent(d) for d in range(1, n_cent)]
    barrier = pltpu.get_barrier_semaphore()
    for peer in peers:
        pl.semaphore_signal(barrier, inc=1, device_id=peer, device_id_type=MESH)

    used = [0]

    def slots(n):
        used[0] += n
        return used[0] - n

    def remote(i, src, dst, dev, s=0):
        return pltpu.make_async_remote_copy(
            src_ref=src,
            dst_ref=dst,
            send_sem=ssem.at[s],
            recv_sem=rsem.at[i],
            device_id=dev,
            device_id_type=MESH,
        )

    def send(i, src, dst, dev, s=0):
        remote(i, src, dst, dev, s).start()

    def wait(sem, ref):
        pltpu.make_async_copy(ref, ref, sem).wait()

    part = n_points // 4

    def load_points(i):
        return pltpu.make_async_copy(
            points.at[i], w.at[0, i], lsem.at[i]
        )

    def load_cents(i):
        slot = lax.rem(i, 2)
        return pltpu.make_async_copy(
            cents.at[pl.ds(i * chunk, chunk)], cstage.at[slot], lsem.at[4 + slot]
        )

    load_points(0).start()
    load_cents(0).start()
    for i in range(1, 4):
        load_points(i).start()
    load_cents(1).start()

    def round_cents(i):
        slot = lax.rem(i, 2)
        value = cstage[slot]
        ch[slot] = value.astype(BF16)
        sqb[slot] = jnp.broadcast_to(
            jnp.sum(value * value, axis=1, keepdims=True) * scale, (chunk, 128)
        )

    def first(c, t, logit):
        slot = lax.rem(c, 2)
        inner = lax.dot_general(
            ch[slot], pt[:, t * tile : (t + 1) * tile], (((1,), (0,)), ((), ())),
            preferred_element_type=F32,
        )
        value = inner * (2.0 * scale) - jnp.concatenate([sqb[slot]] * (tile // 128), axis=1)
        logit[...] = value
        return jnp.max(value, axis=0, keepdims=True)

    def second(c, t, logit, high):
        at = slice(t * tile, (t + 1) * tile)
        e = jnp.exp2(logit[...] - high)
        base = pl.multiple_of(c * chunk, chunk)
        expo[pl.ds(base, chunk), at] = e.astype(BF16)
        mtop[c, :, at] = high
        msum[c, :, at] = jnp.sum(e, axis=0, keepdims=True)

    logits = (logit0, logit1)

    def on_chunk(c, high, last):
        if not last:
            load_cents(c + 1).wait()

            @pl.when(c + 2 < n_chunk)
            def _():
                load_cents(c + 2).start()

        for t in range(n_tile):
            if t + 1 < n_tile:
                after = first(c, t + 1, logits[(t + 1) % 2])
                if t == 0 and not last:
                    round_cents(c + 1)
            elif not last:
                after = first(c + 1, 0, logits[(t + 1) % 2])
            second(c, t, logits[t % 2], high)
            high = after
        return high

    def round_points(i):
        load_points(i).wait()
        half = w[0, i].reshape(part, width).astype(BF16)
        ph[i * part : (i + 1) * part, :] = half
        pt[:, i * part : (i + 1) * part] = half.T

    round_points(0)
    load_cents(0).wait()
    round_cents(0)
    high = first(0, 0, logit0)
    for i in range(1, 4):
        round_points(i)
    high = lax.fori_loop(0, n_chunk - 1, lambda c, high: on_chunk(c, high, False), high)
    on_chunk(n_chunk - 1, high, True)

    stats = slots(1)
    top = functools.reduce(jnp.maximum, [mtop[c] for c in range(n_chunk)])
    total = sum(msum[c] * jnp.exp2(mtop[c] - top) for c in range(n_chunk))
    for i in range(n_points // 128):
        stat[0, i : i + 1, :] = top[:, i * 128 : (i + 1) * 128]
        stat[1, i : i + 1, :] = total[:, i * 128 : (i + 1) * 128]
    pl.semaphore_wait(barrier, len(peers))
    for d in range(1, n_cent):
        send(stats, stat, statr.at[d - 1], at_cent(d), 1)

    def absorb():
        wait(rsem.at[stats], statr)
        tops = [stat[0]] + [statr[d, 0] for d in range(n_cent - 1)]
        sums = [stat[1]] + [statr[d, 1] for d in range(n_cent - 1)]
        high = functools.reduce(jnp.maximum, tops)
        inverse = 1.0 / sum(s * jnp.exp2(t - high) for t, s in zip(tops, sums))
        for i in range(n_points // 128):
            row[0, :, i * 128 : (i + 1) * 128] = high[i : i + 1, :]
            row[1, :, i * 128 : (i + 1) * 128] = inverse[i : i + 1, :]
        for c in range(n_chunk):
            factor[c] = jnp.exp2(mtop[c] - row[0]) * row[1]

    us, vs = (x, z), (z, x)
    fins = []
    for c in range(2):
        for h in range(2):
            at = ((c * 4 + us[c]) * 2 + h) * (4 * rows) + vs[c] * rows
            fins.append(
                pltpu.make_async_copy(
                    cents.at[pl.ds(pl.multiple_of(at, rows), rows)],
                    cfin.at[c, h],
                    lsem.at[6 + 2 * c + h],
                )
            )
            fins[-1].start()

    def produce(pieces):
        spots = []
        for block, b in pieces:
            at = block * (4 * rows) + (0 if b is None else b * rows)
            spots.append((pl.multiple_of(at, rows), lax.div(block * (4 * rows), chunk)))
        size = 4 * rows // len(pieces)
        acc = jnp.zeros((4 * rows, width), F32)
        count = jnp.zeros((4 * rows, 128), F32)
        for t in range(n_tile):
            cols = slice(t * tile, (t + 1) * tile)
            parts = [
                (expo[pl.ds(at, size), cols].astype(F32) * factor[group, :, cols]).astype(BF16)
                for at, group in spots
            ]
            resp = parts[0] if len(parts) == 1 else jnp.concatenate(parts, axis=0)
            acc += jnp.dot(resp, ph[cols, :], preferred_element_type=F32)
            wide = resp.astype(F32)
            for l in range(tile // 128):
                count += wide[:, l * 128 : (l + 1) * 128]
        line = jnp.sum(count.T, axis=0, keepdims=True)
        for k in range(4):
            block, b = pieces[k] if len(pieces) == 4 else (pieces[0][0], k)
            w[lax.div(block, 8), lax.rem(lax.div(block, 2), 4), lax.rem(block, 2), b] = acc[
                k * rows : (k + 1) * rows
            ]
            cnt[block, b, :, :rows] = line[:, k * rows : (k + 1) * rows]

    def block_of(c, bu, h):
        return (c * 4 + bu) * 2 + h

    ups = (at_x(1), at_z(1))
    downs = (at_x(3), at_z(3))
    u = [[lax.rem(us[c] + d, 4) for d in range(4)] for c in range(2)]
    v = [[lax.rem(vs[c] + d, 4) for d in range(4)] for c in range(2)]
    order = (2, 1, 3, 0)

    def place(c):
        return x * (1 - c) + z * c, z * (1 - c) + x * c

    def along(c, d):
        return (lax.rem(z + c * d, 4) * 4 + lax.rem(x + (1 - c) * d, 4), ce)

    far, near = slots(8), slots(1)

    def far_copy(c, h, k):
        here, other = place(c)
        step = lax.rem(2 + 3 * k + lax.div(k, 2) * 3 + lax.div(k, 3) * 2, 4)
        b = lax.rem(other + step, 4)
        return remote(
            far + c * 4 + k,
            w.at[c, lax.rem(here + 2, 4), h, b],
            r1.at[c, h, b],
            along(c, 1 + 2 * h),
        )

    def near_copy(c, h):
        here, _ = place(c)
        d = 3 - 2 * h
        return remote(
            near, w.at[c, lax.rem(here + d, 4), h], r2.at[c, 1 - h, h], along(c, d)
        )

    def farthest(k, carry):
        step = lax.rem(2 + 3 * k + lax.div(k, 2) * 3 + lax.div(k, 3) * 2, 4)
        produce(
            [
                (block_of(c, lax.rem(place(c)[0] + 2, 4), h), lax.rem(place(c)[1] + step, 4))
                for h in range(2)
                for c in range(2)
            ]
        )
        for h in range(2):
            for c in range(2):
                far_copy(c, h, k).start()
        return carry

    def nearest(i, carry):
        c, h = lax.rem(i, 2), 1 - lax.div(i, 2)
        produce([(block_of(c, lax.rem(place(c)[0] + 3 - 2 * h, 4), h), None)])
        near_copy(c, h).start()
        return carry

    def others(i, carry):
        c, h, mine = lax.rem(i, 2), lax.rem(lax.div(i, 2), 2), lax.div(i, 4)
        produce([(block_of(c, lax.rem(place(c)[0] + (1 - mine) * (1 + 2 * h), 4), h), None)])
        return carry

    absorb()
    lax.fori_loop(0, 4, farthest, 0)
    lax.fori_loop(0, 4, nearest, 0)
    lax.fori_loop(0, 8, others, 0)
    xrec = slots(2)
    for d in (1, 2, 3):
        to = lax.rem(x + d, 4)
        send(xrec, cnt.at[pl.ds(2 * to, 2)], cntx0.at[d - 1], at_x(d), 2)
        send(xrec + 1, cnt.at[pl.ds(8, 8), to], cntx1.at[d - 1], at_x(d), 3)

    two, four = w.at[0, 0, 0, pl.ds(0, 2)], w.at[0, 0, 0]
    tail = slots(8)
    for k, d in enumerate(order):
        for c in range(2):
            b = v[c][d]
            wait(rsem.at[far + c * 4 + k], two)
            at = tail + c * 4 + k
            w[c, u[c][1], 0, b] += r1[c, 0, b]
            send(at, w.at[c, u[c][1], 0, b], r2.at[c, 0, 0, b], ups[c])
            w[c, u[c][3], 1, b] += r1[c, 1, b]
            send(at, w.at[c, u[c][3], 1, b], r2.at[c, 1, 1, b], downs[c])
    wait(rsem.at[xrec], cntx0)
    wait(rsem.at[xrec + 1], cntx1)
    mine = pl.ds(2 * x, 2)
    cnt[mine] = cnt[mine] + cntx0[0] + cntx0[1] + cntx0[2]
    cnt[8:16, x] = cnt[8:16, x] + cntx1[0] + cntx1[1] + cntx1[2]
    zrec = slots(1)
    for d in (1, 2, 3):
        to = lax.rem(z + d, 4)
        send(zrec, cnt.at[mine, to], cntz.at[0, d - 1], at_z(d), 4)
        send(zrec, cnt.at[pl.ds(8 + 2 * to, 2), x], cntz.at[1, d - 1], at_z(d), 4)
    wait(rsem.at[near], w.at[0, pl.ds(0, 2)])

    ups2, downs2 = ups[::-1], downs[::-1]
    halves = [pl.ds(q * (rows // 2), rows // 2) for q in range(2)]
    early, ends = slots(4), slots(2)

    def pass_on(c, h, d, q):
        side = h if d is None else 1 - h
        to = (ups2, downs2)[side][c]
        b = v[c][d or (1 + 2 * h)]
        send(
            ends + q, w.at[c, us[c], h, b, halves[q]], t2.at[c, side, h, halves[q]], to
        )

    for k, d in enumerate(order):
        for c in range(2):
            b, me = v[c][d], us[c]
            wait(rsem.at[tail + c * 4 + k], two)
            for h in range(2):
                w[c, me, h, b] += r2[c, 0, h, b] + r2[c, 1, h, b]
            if d == 2:
                for q in range(2):
                    part, at = halves[q], early + 2 * c + q
                    send(at, w.at[c, me, 0, b, part], t1.at[c, 0, part], ups2[c])
                    send(at, w.at[c, me, 1, b, part], t1.at[c, 1, part], downs2[c])
            if d == 1:
                pass_on(c, 1, 1, 0)
            if d == 3:
                pass_on(c, 0, 3, 0)
    for q in range(2):
        if q == 1:
            for c in range(2):
                pass_on(c, 1, 1, 1)
                pass_on(c, 0, 3, 1)
        for c in range(2):
            me, part = us[c], halves[q]
            wait(rsem.at[early + 2 * c + q], w.at[0, 0, 0, 0])
            w[c, me, 0, v[c][1], part] += t1[c, 0, part]
            pass_on(c, 0, None, q)
            w[c, me, 1, v[c][3], part] += t1[c, 1, part]
            pass_on(c, 1, None, q)

    wait(rsem.at[zrec], cntz)
    for copy in fins:
        copy.wait()
    counts = {}
    for c in range(2):
        for h in range(2):
            line = cnt[(c * 4 + us[c]) * 2 + h, vs[c]]
            line = line + cntz[c, 0, h] + cntz[c, 1, h] + cntz[c, 2, h]
            counts[c, h] = jnp.broadcast_to(line, (128, 128)).T + 1.0
    g, h_, f, e, k_ = slots(4), slots(2), slots(2), slots(6), slots(1)
    for q in range(2):
        wait(rsem.at[ends + q], four)
        part = halves[q]
        for c in range(2):
            me, b = us[c], vs[c]
            for h in range(2):
                count = counts[c, h][q * (rows // 2) : (q + 1) * (rows // 2)]
                count = jnp.concatenate([count] * (width // 128), axis=1)
                value = w[c, me, h, b, part] + t2[c, 0, h, part] + t2[c, 1, h, part]
                got[c, me, h, b, part] = (value + cfin[c, h, part]) / count
            piece = got.at[c, me, :, b, part]
            send(g + 2 * c, piece, piece, ups2[c])
            send(g + 2 * c + 1, piece, piece, downs2[c])
        for c in range(2):
            piece = got.at[c, us[c], :, vs[c], part]
            send(h_ + c, piece, piece, ups[c])
            send(h_ + c, piece, piece, downs[c])

    def spread(c, d):
        piece = got.at[c, us[c], :, v[c][d]]
        at = e + 3 * c + d - 1
        send(at, piece, piece, ups[c])
        send(at, piece, piece, downs[c])

    def onward(c, d):
        b = v[c][d]
        wait(rsem.at[h_ + c if d == 0 else e + 3 * c + d - 1], four)
        piece = got.at[c, u[c][3], 0, b]
        send(k_, piece, piece, ups[c])
        piece = got.at[c, u[c][1], 1, b]
        send(k_, piece, piece, downs[c])

    for c in range(2):
        wait(rsem.at[g + 2 * c], two)
        piece = got.at[c, us[c], 0, v[c][3]]
        send(f + c, piece, piece, ups2[c])
        spread(c, 3)
        wait(rsem.at[g + 2 * c + 1], two)
        piece = got.at[c, us[c], 1, v[c][1]]
        send(f + c, piece, piece, downs2[c])
        spread(c, 1)
    for c in range(2):
        onward(c, 0)
    for c in range(2):
        wait(rsem.at[f + c], two)
        spread(c, 2)
    for d in (3, 1, 2):
        for c in range(2):
            onward(c, d)
    wait(rsem.at[k_], w.at[0, pl.ds(0, 2)])
    total_rows = expo.shape[0] * 15 // 16
    wait(ssem.at[0], expo.at[pl.ds(0, total_rows)])
    wait(ssem.at[1], statr)
    wait(ssem.at[2], cntx0)
    wait(ssem.at[3], cntx1)
    wait(ssem.at[4], cntz)


def store(got, out, sem):
    copies = [
        pltpu.make_async_copy(got.at[c, pl.ds(2 * h, 2)], out.at[c, pl.ds(2 * h, 2)], sem.at[2 * c + h])
        for c in range(2)
        for h in range(2)
    ]
    for copy in copies:
        copy.start()
    for copy in copies:
        copy.wait()


def body(points, centroids):
    n_points, width = points.shape
    n_rows = centroids.shape[0]
    n_cent = lax.axis_size("cent")
    chunk, tile = n_rows // 8, 512
    rows = n_rows // 64
    pieces = (2, 4, 2, 4, rows, width)
    n_groups = 1 + 9 + 2 + 8 + 1 + 6 + 15
    vm = pltpu.VMEM
    flat = (n_rows // chunk, 1, n_points)
    scratch = [
        vm((n_points, width), BF16),
        vm((width, n_points), BF16),
        vm((2, chunk, width), F32),
        vm((2, chunk, width), BF16),
        vm((2, chunk, 128), F32),
        vm((chunk, tile), F32),
        vm((chunk, tile), F32),
        vm((n_rows, n_points), BF16),
        vm(flat, F32),
        vm(flat, F32),
        vm(flat, F32),
        vm((2, n_points // 128, 128), F32),
        vm((n_cent - 1, 2, n_points // 128, 128), F32),
        vm((2, 1, n_points), F32),
        vm(pieces, F32),
        vm((2, 2, 4, rows, width), F32),
        vm((2, 2, 2, 4, rows, width), F32),
        vm((2, 2, rows, width), F32),
        vm((2, 2, 2, rows, width), F32),
        vm((2, 2, rows, width), F32),
        vm((16, 4, 1, 128), F32),
        vm((3, 2, 4, 1, 128), F32),
        vm((3, 8, 1, 128), F32),
        vm((2, 3, 2, 1, 128), F32),
        pltpu.SemaphoreType.DMA((5,)),
        pltpu.SemaphoreType.DMA((n_groups,)),
        pltpu.SemaphoreType.DMA((10,)),
    ]
    result = pl.pallas_call(
        functools.partial(kernel, n_cent),
        out_shape=pltpu.VMEM(pieces, F32),
        in_specs=[pl.BlockSpec(memory_space=pl.ANY)] * 2,
        out_specs=pl.BlockSpec(memory_space=pltpu.VMEM),
        scratch_shapes=scratch,
        compiler_params=pltpu.CompilerParams(
            collective_id=0, has_side_effects=True, vmem_limit_bytes=54 * 2**20
        ),
    )(points.reshape(4, 2, 4, n_points // 32, width), centroids)
    saved = pl.pallas_call(
        store,
        out_shape=jax.ShapeDtypeStruct(pieces, F32),
        in_specs=[pl.BlockSpec(memory_space=pltpu.VMEM)],
        out_specs=pl.BlockSpec(memory_space=pl.ANY),
        scratch_shapes=[pltpu.SemaphoreType.DMA((4,))],
        compiler_params=pltpu.CompilerParams(vmem_limit_bytes=2**20),
    )(result)
    return saved.reshape(n_rows, width)


def solution(mesh):
    placed = (P("dp", None), P("cent", None))
    return jax.shard_map(
        body, mesh=mesh, in_specs=placed, out_specs=P("cent", None), check_vma=False
    )
```
